128 devices in a mesh: section: 8 (over z_hi, x), state: 16 (over z_lo, y, core).
Axes of the slice: x: 4, y: 4, z: 4 (z_hi: 2, z_lo: 2; z = z_hi * 2 + z_lo), core: 2. Of those that a mesh axis runs over, the one named last changes fastest.
Arguments:
- belief: float32 [8, 512, 2048], P('section', None, 'state'), may hold values from 0 to 0.04
- action: int32 [8, 512], P('section'), may hold values from 0 to 7
- next_index: int32 [8, 512, 32], P('section'), may hold values from 0 to 511, as said below
- obs_table: float32 [8, 32, 2048], P(None, None, 'state'), may hold values from -1 to 1
- transition: bfloat16 [8, 2048, 2048], P(None, 'state'), may hold values from -0.1875 to 0.1875
- reward: float32 [8, 2048], P(None, 'state'), may hold values from -6 to 6
- terminal: float32 [512, 2048], P(None, 'state'), may hold values from -6 to 6
Outputs:
- alphas: float32 [8, 512, 2048], P('section', None, 'state')
- values: float32 [8, 512], P('section')
The draws below stay inside these ranges and needn't reach their ends.
Inputs may be any that keep to these rules, and one draw needn't show every extreme that they name: next_index[h, b, o] < 128 * (b // 128 + 1): a belief of micro-batch m names only next-section alpha vectors of micro-batches 0 to m.
All inputs are finite; a program needn't handle non-finite values.
Results may differ from the reference program's by a relative error of at most 0.012.
Values sent between devices are 32-bit elements; how exact they have to be, the bound alone decides.
A program may use at most 64 MiB of HBM per device.

```python
import jax
import jax.numpy as jnp
from jax import lax

S = 2048
A = 8
OBS = 32
K = 512
BLOCK = 128
HORIZON = 8


def draw_next_index(key, part):
    rows = jnp.arange(K, dtype=jnp.int32)
    upper = (rows // BLOCK + 1) * BLOCK
    upper = jnp.broadcast_to(upper[None, :, None], (HORIZON, K, OBS))
    return jax.random.randint(jax.random.fold_in(key, 11), (HORIZON, K, OBS), 0, upper, dtype=jnp.int32)


def with_ends(result, key, low, largest):
    spot = [jax.random.randint(jax.random.fold_in(key, axis), (), 0, length) for axis, length in enumerate(result.shape)]
    main_axis = result.shape.index(max(result.shape))
    beside = spot[:main_axis] + [(spot[main_axis] + 1) % result.shape[main_axis]] + spot[main_axis + 1:]
    return result.at[tuple(spot)].set(low).at[tuple(beside)].set(largest)


def raised(entries, stream_key, source, target, shards_of, factor):
    def block_of(dim):
        return (jnp.arange(entries.shape[dim]) // (entries.shape[dim] // shards_of)).reshape((-1,) + (1,) * (entries.ndim - 1 - dim))

    first = jax.random.permutation(stream_key, shards_of)[block_of(target)]
    second = (block_of(target) + shards_of // 2) % shards_of
    return jnp.where((block_of(source) == first) | (block_of(source) == second), factor * entries, entries)


def level_of(key, extent, cuts, least, high):
    loudness = 1.0
    for position, shards_of in cuts:
        draws = jax.random.uniform(jax.random.fold_in(jax.random.fold_in(key, 6), position), (shards_of,), jnp.float32, least / len(cuts), high / len(cuts))
        loudness = loudness * jnp.repeat(jnp.exp(draws), extent[position] // shards_of).reshape((-1,) + (1,) * (len(extent) - 1 - position))
    return loudness


def gaussian(own_key, dims, deviation, reach, cuts=(), held_as=jnp.bfloat16):
    drawn = jax.random.normal(own_key, dims, jnp.float32) * deviation
    if len(cuts) > 0:
        drawn = level_of(own_key, dims, cuts, -0.22, 0.18) * drawn
    return jnp.clip(drawn, min=-reach, max=reach).astype(held_as)


def gaussian_with(rng, extent, width, most, split, heavy, kind=jnp.bfloat16):
    drawn = width * jax.random.normal(rng, extent, jnp.float32)
    if split:
        drawn = drawn * level_of(rng, extent, split, -0.22, 0.18)
    return jnp.clip(raised(drawn, jax.random.fold_in(rng, 3), *heavy), -most, most).astype(kind)


def setup_inputs(seed: int = 0) -> dict:
    key_of = jax.random.split(jax.random.key(seed), 8)
    return {
        "belief": jnp.clip(0.04 * jax.random.uniform(key_of[0], (HORIZON, K, S), jnp.float32) ** level_of(key_of[0], (HORIZON, K, S), ((0, 8), (2, 16)), -0.2, 0.2), 0.0, 0.04),
        "action": with_ends(jax.random.randint(key_of[1], (HORIZON, K), 0, A), jax.random.fold_in(key_of[1], 1), 0, A - 1).astype(jnp.int32),
        "next_index": draw_next_index(jax.random.fold_in(key_of[7], 71), 0),
        "obs_table": gaussian(key_of[3], (A, OBS, S), OBS ** -0.5, 1.0, ((2, 16),), jnp.float32),
        "transition": gaussian_with(key_of[4], (A, S, S), S ** -0.5, 0.1875, ((1, 16),), (1, 2, 16, 2.0)),
        "reward": gaussian(key_of[5], (A, S), 1.0, 6.0, ((1, 16),), jnp.float32),
        "terminal": gaussian(key_of[6], (K, S), 1.0, 6.0, ((1, 16),), jnp.float32),
    }


discount = 0.95


def backup(next_alphas, act_rows, next_rows, obs_table, trans_flat, reward):
    picked = next_alphas[next_rows]
    per_action = jnp.einsum('bos,aos->bas', picked, obs_table, precision=lax.Precision.HIGHEST)
    onehot = (act_rows[:, None] == jnp.arange(A, dtype=jnp.int32)[None, :]).astype(jnp.float32)
    masked = (per_action * onehot[:, :, None]).astype(jnp.bfloat16).reshape(act_rows.shape[0], A * S)
    summed = jnp.dot(masked, trans_flat, preferred_element_type=jnp.float32)
    reward_rows = jnp.dot(onehot, reward, precision=lax.Precision.HIGHEST)
    return reward_rows + discount * summed


def reference(belief, action, next_index, obs_table, transition, reward, terminal):
    trans_flat = transition.reshape(A * S, S)
    nextset = terminal
    alpha_list = [None] * HORIZON
    value_list = [None] * HORIZON
    for section_number in reversed(range(HORIZON)):
        act_blocks = action[section_number].reshape(K // BLOCK, BLOCK)
        next_blocks = next_index[section_number].reshape(K // BLOCK, BLOCK, OBS)

        def one_block(pieces, nextset=nextset):
            return backup(nextset, pieces[0], pieces[1], obs_table, trans_flat, reward)

        section_alphas = lax.map(one_block, (act_blocks, next_blocks)).reshape(K, S)
        alpha_list[section_number] = section_alphas
        value_list[section_number] = jnp.sum(belief[section_number] * section_alphas, axis=1)
        nextset = section_alphas
    return jnp.stack(alpha_list), jnp.stack(value_list)
```

```python
import jax
import jax.numpy as jnp
from jax import lax
from jax.experimental import pallas as pl
from jax.experimental.pallas import tpu as pltpu
from jax.sharding import PartitionSpec as P

MESH = pl.DeviceIdType.MESH
discount = 0.95

ACTIONS = 8
OBS = 32
STEPS = 8
SECTIONS = 8
PLANES = 4
CHIPS = 8
SHARDS = 16
BELIEFS = 512
ROWS = 64
W = 128
GROUP = 8


def kernel(
    tab_ref, obs_ref, reward_ref, terminal_ref, trans_hbm, belief_hbm,
    alphas_ref, values_ref,
    trans, belief, nbuf, final, idx, onehot, weight, rewrow, masked,
    pair_send, pair_recv, part_send, part_recv, vbuf,
    load_sem, idx_ssem, idx_rsem, pair_ssem, pair_rsem, part_ssem, part_rsem,
    row_ssem, row_rsem, out_ssem, out_rsem, val_ssem, val_rsem,
):
    sec = lax.axis_index("section")
    st = lax.axis_index("state")
    plane, half = lax.rem(sec, PLANES), lax.div(sec, PLANES)
    core, chip = lax.rem(st, 2), lax.div(st, 2)
    my_chip_lo, my_chip_y = lax.div(chip, 4), lax.rem(chip, 4)

    def rows_of(s):
        return pl.ds(pl.multiple_of((lax.rem(s, PLANES) * 2 + lax.div(s, PLANES)) * ROWS, ROWS), ROWS)

    my_rows = rows_of(sec)

    trans_load = pltpu.make_async_copy(trans_hbm, trans, load_sem.at[0])
    trans_load.start()
    belief_load = pltpu.make_async_copy(belief_hbm, belief, load_sem.at[1])
    belief_load.start()

    def other_section(d):
        return lax.rem(sec + d, SECTIONS)

    def other_state(d):
        return lax.rem(st + d, SHARDS)

    @pl.loop(1, STEPS)
    def _(t):
        nbuf[t] = jnp.zeros((BELIEFS, W), jnp.float32)

    barrier = pltpu.get_barrier_semaphore()
    for d in range(1, SECTIONS):
        pl.semaphore_signal(barrier, inc=1, device_id={"section": other_section(d), "state": st}, device_id_type=MESH)
    for d in range(1, SHARDS):
        pl.semaphore_signal(barrier, inc=1, device_id={"section": sec, "state": other_state(d)}, device_id_type=MESH)
    pl.semaphore_wait(barrier, SECTIONS + SHARDS - 2)

    def idx_copy(d):
        to = other_section(d)
        return pltpu.make_async_remote_copy(
            src_ref=tab_ref.at[rows_of(to)], dst_ref=idx.at[sec],
            send_sem=idx_ssem.at[d], recv_sem=idx_rsem.at[sec],
            device_id={"section": to, "state": st}, device_id_type=MESH,
        )

    for d in range(1, SECTIONS):
        idx_copy(d).start()
    idx[pl.ds(sec, 1)] = tab_ref[my_rows][None]
    nbuf[0] = terminal_ref[...]

    def wait_idx(h):
        @pl.when(h != sec)
        def _():
            pltpu.make_async_remote_copy(
                src_ref=idx.at[h], dst_ref=idx.at[h], send_sem=idx_ssem.at[0], recv_sem=idx_rsem.at[h],
                device_id={"section": sec, "state": other_state(1)}, device_id_type=MESH,
            ).wait_recv()

    def prepare(t):
        h = STEPS - 1 - t
        wait_idx(h)
        table = idx[h]
        act = table[:, OBS : OBS + 1]
        row = jnp.zeros((ROWS, W), jnp.float32)
        for a in range(ACTIONS):
            row = jnp.where(act == a, reward_ref[a : a + 1, :], row)
        rewrow[...] = row
        wide = jnp.broadcast_to(act, (ROWS, W))
        column = lax.broadcasted_iota(jnp.int32, (ROWS, BELIEFS), 1)
        for o in range(OBS):
            pick = table[:, o : o + 1]
            onehot[o * ROWS : (o + 1) * ROWS, :] = (
                jnp.where(column == pick, 1.0, 0.0).astype(jnp.bfloat16)
            )
            w = jnp.zeros((ROWS, W), jnp.float32)
            for a in range(ACTIONS):
                w = jnp.where(wide == a, obs_ref[a, o : o + 1, :], w)
            weight[o] = w

    def chip_at(lo, y):
        return lax.rem(my_chip_lo + lo, 2) * 4 + lax.rem(my_chip_y + y, 4)

    order = ((1, 2), (0, 2), (1, 1), (1, 3), (0, 1), (0, 3), (1, 0), (0, 0))

    def pair_copy(k, t):
        return pltpu.make_async_remote_copy(
            src_ref=pair_send.at[k], dst_ref=pair_recv.at[t, k],
            send_sem=pair_ssem.at[k], recv_sem=pair_rsem.at[t, k],
            device_id={"section": sec, "state": chip * 2 + 1 - core}, device_id_type=MESH,
        )

    def part_copy(k, t):
        return pltpu.make_async_remote_copy(
            src_ref=part_send.at[k], dst_ref=part_recv.at[t, k],
            send_sem=part_ssem.at[k], recv_sem=part_rsem.at[t, k],
            device_id={"section": sec, "state": chip_at(*order[k]) * 2 + core}, device_id_type=MESH,
        )

    def row_copy(d, t):
        to = other_section(d)
        return pltpu.make_async_remote_copy(
            src_ref=nbuf.at[t + 1, my_rows], dst_ref=nbuf.at[t + 1, my_rows],
            send_sem=row_ssem.at[d], recv_sem=row_rsem.at[t, sec],
            device_id={"section": to, "state": st}, device_id_type=MESH,
        )

    def goes_to(d, t):
        to = other_section(d)
        p, f = lax.rem(to, PLANES), lax.div(to, PLANES)
        feeds = (p > plane) | ((p == plane) & (f != half))
        return feeds & (t < STEPS - 1)

    def out_copy(t):
        return pltpu.make_async_remote_copy(
            src_ref=nbuf.at[t + 1, my_rows], dst_ref=final.at[my_rows],
            send_sem=out_ssem, recv_sem=out_rsem.at[sec],
            device_id={"section": STEPS - 1 - t, "state": st}, device_id_type=MESH,
        )

    def wait_rows(source, t):
        pltpu.make_async_remote_copy(
            src_ref=nbuf.at[t + 1, rows_of(source)], dst_ref=nbuf.at[t + 1, rows_of(source)],
            send_sem=row_ssem.at[0], recv_sem=row_rsem.at[t, source],
            device_id={"section": source, "state": st}, device_id_type=MESH,
        ).wait_recv()

    def wait_sent(t):
        for d in range(1, SECTIONS):
            @pl.when(goes_to(d, t))
            def _():
                row_copy(d, t).wait_send()

        @pl.when(STEPS - 1 - t != sec)
        def _():
            out_copy(t).wait_send()

    prepare(0)
    trans_load.wait()

    def step(t, carry):
        following = nbuf[t]
        high = following.astype(jnp.bfloat16)
        low = (following - high.astype(jnp.float32)).astype(jnp.bfloat16)
        both = jnp.concatenate([high, low], axis=1)
        total = jnp.zeros((ROWS, W), jnp.float32)
        for c in range(OBS // GROUP):
            got = jnp.dot(
                onehot[c * GROUP * ROWS : (c + 1) * GROUP * ROWS, :], both,
                preferred_element_type=jnp.float32,
            )
            got = (got[:, :W] + got[:, W:]).reshape(GROUP, ROWS, W)
            total = total + jnp.sum(got * weight[c * GROUP : (c + 1) * GROUP], axis=0)
        act = idx[STEPS - 1 - t][:, OBS : OBS + 1]
        for a in range(ACTIONS):
            masked[:, a * W : (a + 1) * W] = jnp.where(act == a, total, 0.0).astype(jnp.bfloat16)

        mine = []
        for k in range(CHIPS):
            q = chip_at(*order[k])
            part = jnp.dot(
                masked[...], trans[:, pl.ds(pl.multiple_of(q * 2 * W, 2 * W), 2 * W)],
                preferred_element_type=jnp.float32,
            )
            pair_send[k] = jnp.where(core == 0, part[:, W:], part[:, :W])
            pair_copy(k, t).start()
            part_send[k] = jnp.where(core == 0, part[:, :W], part[:, W:])
        for k in range(CHIPS):
            pair_copy(k, t).wait_recv()
            part_send[k] = part_send[k] + pair_recv[t, k]
            if k < CHIPS - 1:
                part_copy(k, t).start()

        reward_part = rewrow[...]

        @pl.when(t < STEPS - 1)
        def _():
            prepare(t + 1)

        summed = part_send[CHIPS - 1]
        for k in range(CHIPS - 1):
            part_copy(k, t).wait_recv()
            summed = summed + part_recv[t, k]
        for k in range(CHIPS):
            pair_copy(k, t).wait_send()

        @pl.when(t > 0)
        def _():
            wait_sent(t - 1)

        fresh = reward_part + discount * summed
        nbuf[t + 1, my_rows] = fresh
        for d in range(1, SECTIONS):
            @pl.when(goes_to(d, t))
            def _():
                row_copy(d, t).start()

        @pl.when(STEPS - 1 - t != sec)
        def _():
            out_copy(t).start()

        @pl.when(STEPS - 1 - t == sec)
        def _():
            final[my_rows] = fresh

        for k in range(CHIPS - 1):
            part_copy(k, t).wait_send()

        @pl.when(t < STEPS - 1)
        def _():
            for d in range(1, SECTIONS):
                source = other_section(d)
                p, f = lax.rem(source, PLANES), lax.div(source, PLANES)

                @pl.when((p < plane) | ((p == plane) & (f != half)))
                def _():
                    wait_rows(source, t)

        return carry

    lax.fori_loop(0, STEPS, step, 0)

    for d in range(1, SECTIONS):
        source = other_section(d)
        pltpu.make_async_remote_copy(
            src_ref=final.at[rows_of(source)], dst_ref=final.at[rows_of(source)],
            send_sem=out_ssem, recv_sem=out_rsem.at[source],
            device_id={"section": source, "state": st}, device_id_type=MESH,
        ).wait_recv()

    belief_load.wait()
    alphas_ref[...] = final[...]
    product = final[...] * belief[...]
    for g in range(BELIEFS // W):
        block = product[g * W : (g + 1) * W, :].T
        vbuf[pl.ds(st, 1), g : g + 1, :] = jnp.sum(block, axis=0, keepdims=True)[None]

    def val_copy(d):
        return pltpu.make_async_remote_copy(
            src_ref=vbuf.at[st], dst_ref=vbuf.at[st],
            send_sem=val_ssem.at[d], recv_sem=val_rsem.at[d],
            device_id={"section": sec, "state": other_state(d)}, device_id_type=MESH,
        )

    for d in range(1, SHARDS):
        val_copy(d).start()
    wait_sent(STEPS - 1)
    for d in range(1, SECTIONS):
        idx_copy(d).wait_send()
    for d in range(1, SHARDS):
        val_copy(d).wait_recv()
    value = vbuf[0]
    for s in range(1, SHARDS):
        value = value + vbuf[s]
    values_ref[...] = value
    for d in range(1, SHARDS):
        val_copy(d).wait_send()


def local(belief, action, next_index, obs_table, transition, reward, terminal):
    table = jnp.concatenate([next_index[0], action[0][:, None]], axis=1)
    table = jnp.pad(table, ((0, 0), (0, W - OBS - 1)))
    vmem = pl.BlockSpec(memory_space=pltpu.VMEM)
    anywhere = pl.BlockSpec(memory_space=pl.ANY)
    dma = pltpu.SemaphoreType.DMA
    alphas, values = pl.pallas_call(
        kernel,
        out_shape=(
            jax.ShapeDtypeStruct((BELIEFS, W), jnp.float32),
            jax.ShapeDtypeStruct((BELIEFS // W, W), jnp.float32),
        ),
        in_specs=[vmem, vmem, vmem, vmem, anywhere, anywhere],
        out_specs=(vmem, vmem),
        scratch_shapes=[
            pltpu.VMEM((ACTIONS * W, SHARDS * W), jnp.bfloat16),
            pltpu.VMEM((BELIEFS, W), jnp.float32),
            pltpu.VMEM((STEPS + 1, BELIEFS, W), jnp.float32),
            pltpu.VMEM((BELIEFS, W), jnp.float32),
            pltpu.VMEM((SECTIONS, ROWS, W), jnp.int32),
            pltpu.VMEM((OBS * ROWS, BELIEFS), jnp.bfloat16),
            pltpu.VMEM((OBS, ROWS, W), jnp.float32),
            pltpu.VMEM((ROWS, W), jnp.float32),
            pltpu.VMEM((ROWS, ACTIONS * W), jnp.bfloat16),
            pltpu.VMEM((CHIPS, ROWS, W), jnp.float32),
            pltpu.VMEM((STEPS, CHIPS, ROWS, W), jnp.float32),
            pltpu.VMEM((CHIPS, ROWS, W), jnp.float32),
            pltpu.VMEM((STEPS, CHIPS, ROWS, W), jnp.float32),
            pltpu.VMEM((SHARDS, BELIEFS // W, W), jnp.float32),
            dma((2,)),
            dma((SECTIONS,)),
            dma((SECTIONS,)),
            dma((CHIPS,)),
            dma((STEPS, CHIPS)),
            dma((CHIPS,)),
            dma((STEPS, CHIPS)),
            dma((SECTIONS,)),
            dma((STEPS, SECTIONS)),
            dma,
            dma((SECTIONS,)),
            dma((SHARDS,)),
            dma((SHARDS,)),
        ],
        compiler_params=pltpu.CompilerParams(
            collective_id=0, has_side_effects=True, vmem_limit_bytes=60 * 1024 * 1024
        ),
        name="chain",
    )(
        table, obs_table, reward, terminal,
        transition.reshape(ACTIONS * W, SHARDS * W), belief[0],
    )
    return alphas[None], values.reshape(1, BELIEFS)


def solution(mesh):
    return jax.shard_map(
        local,
        mesh=mesh,
        in_specs=(
            P("section", None, "state"),
            P("section", None),
            P("section", None, None),
            P(None, None, "state"),
            P(None, "state", None),
            P(None, "state"),
            P(None, "state"),
        ),
        out_specs=(P("section", None, "state"), P("section", None)),
        check_vma=False,
    )
```

```python
import jax
import jax.numpy as jnp
from jax import lax
from jax.experimental import pallas as pl
from jax.experimental.pallas import tpu as pltpu
from jax.sharding import PartitionSpec as P

MESH = pl.DeviceIdType.MESH
discount = 0.95

ACTIONS = 8
OBS = 32
STEPS = 8
SECTIONS = 8
PLANES = 4
CHIPS = 8
SHARDS = 16
BELIEFS = 512
BATCH = 128
ROWS = 64
W = 128
TAB = 40
GROUP = 8


def kernel(
    next_ref, action_ref, reward_ref, obs_hbm, terminal_hbm, trans_hbm, belief_hbm,
    final, vbuf,
    obs, trans, belief, nbuf, tab, idx, turned, onehot, weight, rewrow, masked,
    pair_send, pair_recv, part_send, part_recv, sums_send, sums,
    load_sem, idx_ssem, idx_rsem, pair_ssem, pair_rsem, part_ssem, part_rsem,
    sums_ssem, sums_rsem, row_ssem, row_rsem, out_ssem, out_rsem, val_ssem, val_rsem,
):
    sec = lax.axis_index("section")
    st = lax.axis_index("state")
    plane, half = lax.rem(sec, PLANES), lax.div(sec, PLANES)
    core, chip = lax.rem(st, 2), lax.div(st, 2)
    lo, y = lax.div(chip, 4), lax.rem(chip, 4)

    def rows_of(p):
        return pl.ds(pl.multiple_of(p * BATCH, BATCH), BATCH)

    def other_section(d):
        return lax.rem(sec + d, SECTIONS)

    def other_state(d):
        return lax.rem(st + d, SHARDS)

    def other_plane(d):
        return lax.rem(plane + d, PLANES)

    def z_neighbour(up):
        z = lax.rem(half * 2 + lo + (1 if up else 3), 4)
        return {"section": lax.div(z, 2) * PLANES + plane, "state": (lax.rem(z, 2) * 4 + y) * 2 + core}

    loads = [
        pltpu.make_async_copy(obs_hbm, obs, load_sem.at[0]),
        pltpu.make_async_copy(terminal_hbm, nbuf.at[0], load_sem.at[1]),
        pltpu.make_async_copy(trans_hbm, trans, load_sem.at[2]),
        pltpu.make_async_copy(belief_hbm, belief, load_sem.at[3]),
    ]
    for load in loads:
        load.start()

    barrier = pltpu.get_barrier_semaphore()
    for d in range(1, SECTIONS):
        pl.semaphore_signal(barrier, inc=1, device_id={"section": other_section(d), "state": st}, device_id_type=MESH)
    for d in range(1, SHARDS):
        pl.semaphore_signal(barrier, inc=1, device_id={"section": sec, "state": other_state(d)}, device_id_type=MESH)
    for up in (True, False):
        pl.semaphore_signal(barrier, inc=1, device_id=z_neighbour(up), device_id_type=MESH)

    for p in range(PLANES):
        tab[p, 0:OBS, :] = next_ref[:, p * BATCH : (p + 1) * BATCH]
        tab[p, OBS : OBS + 1, :] = action_ref[:, p * BATCH : (p + 1) * BATCH]
        tab[p, OBS + 1 :, :] = jnp.zeros((TAB - OBS - 1, BATCH), jnp.int32)
        for t in range(1, STEPS):
            @pl.when(p > plane)
            def _():
                nbuf[t, p * BATCH : (p + 1) * BATCH, :] = jnp.zeros((BATCH, W), jnp.float32)
    idx[pl.ds(sec, 1)] = tab[pl.ds(plane, 1)]

    pl.semaphore_wait(barrier, SECTIONS + SHARDS)

    def idx_copy(d):
        to = other_section(d)
        return pltpu.make_async_remote_copy(
            src_ref=tab.at[lax.rem(to, PLANES)], dst_ref=idx.at[sec],
            send_sem=idx_ssem.at[d], recv_sem=idx_rsem.at[sec],
            device_id={"section": to, "state": st}, device_id_type=MESH,
        )

    for d in range(1, SECTIONS):
        idx_copy(d).start()

    def prepare(t):
        h = STEPS - 1 - t

        @pl.when(h != sec)
        def _():
            pltpu.make_async_remote_copy(
                src_ref=idx.at[h], dst_ref=idx.at[h], send_sem=idx_ssem.at[0], recv_sem=idx_rsem.at[h],
                device_id={"section": sec, "state": other_state(1)}, device_id_type=MESH,
            ).wait_recv()

        turned[...] = idx[h].T
        act = turned[:, OBS : OBS + 1]
        row = jnp.zeros((BATCH, W), jnp.float32)
        for a in range(ACTIONS):
            row = jnp.where(act == a, reward_ref[a : a + 1, :], row)
        rewrow[lax.rem(t, 2)] = row
        table = turned[pl.ds(pl.multiple_of(half * ROWS, ROWS), ROWS), :]
        wide = jnp.broadcast_to(table[:, OBS : OBS + 1], (ROWS, W))
        column = lax.broadcasted_iota(jnp.int32, (ROWS, BELIEFS), 1)
        for o in range(OBS):
            pick = table[:, o : o + 1]
            onehot[o * ROWS : (o + 1) * ROWS, :] = (
                jnp.where(column == pick, 1.0, 0.0).astype(jnp.bfloat16)
            )
            w = jnp.zeros((ROWS, W), jnp.float32)
            for a in range(ACTIONS):
                w = jnp.where(wide == a, obs[a, o : o + 1, :], w)
            weight[o] = w

    order = ((1, 2), (0, 2), (1, 1), (1, 3), (0, 1), (0, 3), (1, 0), (0, 0))

    def chip_at(k, flip):
        return lax.rem(lo + order[k][0] + flip, 2) * 4 + lax.rem(y + order[k][1], 4)

    def pair_copy(k, t):
        return pltpu.make_async_remote_copy(
            src_ref=pair_send.at[k], dst_ref=pair_recv.at[t, k],
            send_sem=pair_ssem.at[k], recv_sem=pair_rsem.at[t, k],
            device_id={"section": sec, "state": chip * 2 + 1 - core}, device_id_type=MESH,
        )

    def part_copy(k, t):
        return pltpu.make_async_remote_copy(
            src_ref=part_send.at[k], dst_ref=part_recv.at[t, k],
            send_sem=part_ssem.at[k], recv_sem=part_rsem.at[t, k],
            device_id={"section": sec, "state": chip_at(k, 0) * 2 + core}, device_id_type=MESH,
        )

    def sums_copy(up, t):
        return pltpu.make_async_remote_copy(
            src_ref=sums_send, dst_ref=sums.at[t, half],
            send_sem=sums_ssem.at[int(up)], recv_sem=sums_rsem.at[t, half],
            device_id=z_neighbour(up), device_id_type=MESH,
        )

    def wait_sums(f, t):
        pltpu.make_async_remote_copy(
            src_ref=sums_send, dst_ref=sums.at[t, f],
            send_sem=sums_ssem.at[0], recv_sem=sums_rsem.at[t, f],
            device_id=z_neighbour(True), device_id_type=MESH,
        ).wait_recv()

    def row_copy(d, t):
        return pltpu.make_async_remote_copy(
            src_ref=nbuf.at[t + 1, rows_of(plane)], dst_ref=nbuf.at[t + 1, rows_of(plane)],
            send_sem=row_ssem.at[d], recv_sem=row_rsem.at[t, plane],
            device_id={"section": half * PLANES + other_plane(d), "state": st}, device_id_type=MESH,
        )

    def feeds(d, t):
        return (other_plane(d) > plane) & (t < STEPS - 1)

    def wait_rows(p, t):
        pltpu.make_async_remote_copy(
            src_ref=nbuf.at[t + 1, rows_of(p)], dst_ref=nbuf.at[t + 1, rows_of(p)],
            send_sem=row_ssem.at[0], recv_sem=row_rsem.at[t, p],
            device_id={"section": half * PLANES + other_plane(1), "state": st}, device_id_type=MESH,
        ).wait_recv()

    def out_copy(t):
        return pltpu.make_async_remote_copy(
            src_ref=nbuf.at[t + 1, rows_of(plane)], dst_ref=final.at[rows_of(plane)],
            send_sem=out_ssem, recv_sem=out_rsem.at[plane],
            device_id={"section": STEPS - 1 - t, "state": st}, device_id_type=MESH,
        )

    def goes_out(t):
        owner = STEPS - 1 - t
        return (lax.div(owner, PLANES) == half) & (lax.rem(owner, PLANES) < plane)

    def wait_sent(t):
        for d in range(1, PLANES):
            @pl.when(feeds(d, t))
            def _():
                row_copy(d, t).wait_send()

        @pl.when(goes_out(t))
        def _():
            out_copy(t).wait_send()

    loads[0].wait()
    prepare(0)
    loads[1].wait()
    loads[2].wait()

    def step(t, carry):
        following = nbuf[t]
        high = following.astype(jnp.bfloat16)
        low = (following - high.astype(jnp.float32)).astype(jnp.bfloat16)
        both = jnp.concatenate([high, low], axis=1)
        total = jnp.zeros((ROWS, W), jnp.float32)
        for c in range(OBS // GROUP):
            got = jnp.dot(
                onehot[c * GROUP * ROWS : (c + 1) * GROUP * ROWS, :], both,
                preferred_element_type=jnp.float32,
            )
            got = (got[:, :W] + got[:, W:]).reshape(GROUP, ROWS, W)
            total = total + jnp.sum(got * weight[c * GROUP : (c + 1) * GROUP], axis=0)
        act = turned[pl.ds(pl.multiple_of(half * ROWS, ROWS), ROWS), :][:, OBS : OBS + 1]
        for a in range(ACTIONS):
            masked[:, a * W : (a + 1) * W] = jnp.where(act == a, total, 0.0).astype(jnp.bfloat16)

        for k in range(CHIPS):
            part = jnp.dot(
                masked[...], trans[:, pl.ds(pl.multiple_of(chip_at(k, 1) * 2 * W, 2 * W), 2 * W)],
                preferred_element_type=jnp.float32,
            )
            pair_send[k] = jnp.where(core == 0, part[:, W:], part[:, :W])
            pair_copy(k, t).start()
            part_send[k] = jnp.where(core == 0, part[:, :W], part[:, W:])
        for k in range(CHIPS):
            pair_copy(k, t).wait_recv()
            part_send[k] = part_send[k] + pair_recv[t, k]
            if k < CHIPS - 1:
                part_copy(k, t).start()

        @pl.when(t > 0)
        def _():
            wait_sent(t - 1)

        @pl.when(t < STEPS - 1)
        def _():
            prepare(t + 1)

        for k in range(CHIPS):
            pair_copy(k, t).wait_send()
        summed = part_send[CHIPS - 1]
        for k in range(CHIPS - 1):
            part_copy(k, t).wait_recv()
            summed = summed + part_recv[t, k]
        sums_send[...] = summed
        for up in (True, False):
            sums_copy(up, t).start()
        for k in range(CHIPS - 1):
            part_copy(k, t).wait_send()
        for f in (0, 1):
            wait_sums(f, t)
        nbuf[t + 1, rows_of(plane)] = (
            rewrow[lax.rem(t, 2)] + discount * sums[t].reshape(BATCH, W)
        )
        for d in range(1, PLANES):
            @pl.when(feeds(d, t))
            def _():
                row_copy(d, t).start()

        @pl.when(goes_out(t))
        def _():
            out_copy(t).start()

        for up in (True, False):
            sums_copy(up, t).wait_send()

        @pl.when(t < STEPS - 1)
        def _():
            for p in range(PLANES - 1):
                @pl.when(p < plane)
                def _():
                    wait_rows(p, t)

        return carry

    lax.fori_loop(0, STEPS, step, 0)

    own = STEPS - 1 - sec
    for p in range(PLANES):
        @pl.when(p <= plane)
        def _():
            final[p * BATCH : (p + 1) * BATCH, :] = nbuf[own + 1, p * BATCH : (p + 1) * BATCH, :]

    loads[3].wait()
    for p in range(PLANES):
        @pl.when(p > plane)
        def _():
            pltpu.make_async_remote_copy(
                src_ref=final.at[rows_of(p)], dst_ref=final.at[rows_of(p)],
                send_sem=out_ssem, recv_sem=out_rsem.at[p],
                device_id={"section": half * PLANES + other_plane(1), "state": st}, device_id_type=MESH,
            ).wait_recv()

        block = final[p * BATCH : (p + 1) * BATCH, :] * belief[p * BATCH : (p + 1) * BATCH, :]
        vbuf[pl.ds(st, 1), p : p + 1, :] = jnp.sum(block.T, axis=0, keepdims=True)[None]

    def val_copy(d):
        return pltpu.make_async_remote_copy(
            src_ref=vbuf.at[st], dst_ref=vbuf.at[st],
            send_sem=val_ssem.at[d], recv_sem=val_rsem.at[d],
            device_id={"section": sec, "state": other_state(d)}, device_id_type=MESH,
        )

    for d in range(1, SHARDS):
        val_copy(d).start()
    wait_sent(STEPS - 1)
    for d in range(1, SECTIONS):
        idx_copy(d).wait_send()
    for d in range(1, SHARDS):
        val_copy(d).wait_recv()
    for d in range(1, SHARDS):
        val_copy(d).wait_send()


def finish(final_ref, vbuf_ref, alphas_ref, values_ref):
    alphas_ref[...] = final_ref[...]
    value = vbuf_ref[0]
    for s in range(1, SHARDS):
        value = value + vbuf_ref[s]
    values_ref[...] = value


def local(belief, action, next_index, obs_table, transition, reward, terminal):
    vmem = pl.BlockSpec(memory_space=pltpu.VMEM)
    anywhere = pl.BlockSpec(memory_space=pl.ANY)
    dma = pltpu.SemaphoreType.DMA
    f32 = jnp.float32
    final, parts = pl.pallas_call(
        kernel,
        out_shape=(
            jax.ShapeDtypeStruct((BELIEFS, W), f32),
            jax.ShapeDtypeStruct((SHARDS, PLANES, W), f32),
        ),
        in_specs=[vmem, vmem, vmem, anywhere, anywhere, anywhere, anywhere],
        out_specs=(vmem, vmem),
        scratch_shapes=[
            pltpu.VMEM((ACTIONS, OBS, W), f32),
            pltpu.VMEM((ACTIONS * W, SHARDS * W), jnp.bfloat16),
            pltpu.VMEM((BELIEFS, W), f32),
            pltpu.VMEM((STEPS + 1, BELIEFS, W), f32),
            pltpu.VMEM((PLANES, TAB, BATCH), jnp.int32),
            pltpu.VMEM((SECTIONS, TAB, BATCH), jnp.int32),
            pltpu.VMEM((BATCH, TAB), jnp.int32),
            pltpu.VMEM((OBS * ROWS, BELIEFS), jnp.bfloat16),
            pltpu.VMEM((OBS, ROWS, W), f32),
            pltpu.VMEM((2, BATCH, W), f32),
            pltpu.VMEM((ROWS, ACTIONS * W), jnp.bfloat16),
            pltpu.VMEM((CHIPS, ROWS, W), f32),
            pltpu.VMEM((STEPS, CHIPS, ROWS, W), f32),
            pltpu.VMEM((CHIPS, ROWS, W), f32),
            pltpu.VMEM((STEPS, CHIPS, ROWS, W), f32),
            pltpu.VMEM((ROWS, W), f32),
            pltpu.VMEM((STEPS, 2, ROWS, W), f32),
            dma((4,)),
            dma((SECTIONS,)),
            dma((SECTIONS,)),
            dma((CHIPS,)),
            dma((STEPS, CHIPS)),
            dma((CHIPS,)),
            dma((STEPS, CHIPS)),
            dma((2,)),
            dma((STEPS, 2)),
            dma((PLANES,)),
            dma((STEPS, PLANES)),
            dma,
            dma((PLANES,)),
            dma((SHARDS,)),
            dma((SHARDS,)),
        ],
        compiler_params=pltpu.CompilerParams(
            collective_id=0, has_side_effects=True, vmem_limit_bytes=60 * 1024 * 1024
        ),
        name="chain",
    )(
        next_index[0].T, action, reward, obs_table, terminal,
        transition.reshape(ACTIONS * W, SHARDS * W), belief[0],
    )
    alphas, values = pl.pallas_call(
        finish,
        out_shape=(
            jax.ShapeDtypeStruct((BELIEFS, W), f32),
            jax.ShapeDtypeStruct((PLANES, W), f32),
        ),
        in_specs=[vmem, vmem],
        out_specs=(vmem, vmem),
        name="finish",
    )(final, parts)
    return alphas[None], values.reshape(1, BELIEFS)


def solution(mesh):
    return jax.shard_map(
        local,
        mesh=mesh,
        in_specs=(
            P("section", None, "state"),
            P("section", None),
            P("section", None, None),
            P(None, None, "state"),
            P(None, "state", None),
            P(None, "state"),
            P(None, "state"),
        ),
        out_specs=(P("section", None, "state"), P("section", None)),
        check_vma=False,
    )
```

```python
import jax
import jax.numpy as jnp
from jax import lax
from jax.experimental import pallas as pl
from jax.experimental.pallas import tpu as pltpu
from jax.sharding import PartitionSpec as P

MESH = pl.DeviceIdType.MESH
discount = 0.95

ACTIONS = 8
OBS = 32
STEPS = 8
SECTIONS = 8
PLANES = 4
CHIPS = 8
SHARDS = 16
BELIEFS = 512
BATCH = 128
ROWS = 64
W = 128
TAB = 40
GROUP = 8


def kernel(
    next_ref, action_ref, reward_ref, obs_hbm, terminal_hbm, trans_hbm, belief_hbm,
    final, vbuf,
    obs, trans, belief, nbuf, tab, idx, turned, onehot, weight, reward, rewrow, masked,
    pair_send, pair_recv, part_send, part_recv, fresh,
    load_sem, idx_ssem, idx_rsem, reward_ssem, reward_rsem, pair_ssem, pair_rsem, part_ssem, part_rsem,
    row_ssem, row_rsem, out_ssem, out_rsem, val_ssem, val_rsem,
):
    sec = lax.axis_index("section")
    st = lax.axis_index("state")
    plane, half = lax.rem(sec, PLANES), lax.div(sec, PLANES)
    core, chip = lax.rem(st, 2), lax.div(st, 2)
    lo, y = lax.div(chip, 4), lax.rem(chip, 4)

    mine = plane * 2 + half

    def rows_of(m):
        return pl.ds(pl.multiple_of(m * ROWS, ROWS), ROWS)

    def other_section(d):
        return lax.rem(sec + d, SECTIONS)

    def other_state(d):
        return lax.rem(st + d, SHARDS)

    def z_neighbour(up, d):
        z = lax.rem(half * 2 + lo + (1 if up else 3), 4)
        return {
            "section": lax.div(z, 2) * PLANES + lax.rem(plane + d, PLANES),
            "state": (lax.rem(z, 2) * 4 + y) * 2 + core,
        }

    loads = [
        pltpu.make_async_copy(obs_hbm, obs, load_sem.at[0]),
        pltpu.make_async_copy(terminal_hbm, nbuf.at[0], load_sem.at[1]),
        pltpu.make_async_copy(trans_hbm, trans, load_sem.at[2]),
        pltpu.make_async_copy(belief_hbm, belief, load_sem.at[3]),
    ]
    for load in loads:
        load.start()

    barrier = pltpu.get_barrier_semaphore()
    for d in range(1, SECTIONS):
        pl.semaphore_signal(barrier, inc=1, device_id={"section": other_section(d), "state": st}, device_id_type=MESH)
    for d in range(1, SHARDS):
        pl.semaphore_signal(barrier, inc=1, device_id={"section": sec, "state": other_state(d)}, device_id_type=MESH)
    for up in (True, False):
        for d in range(PLANES):
            pl.semaphore_signal(barrier, inc=1, device_id=z_neighbour(up, d), device_id_type=MESH)

    for p in range(PLANES):
        tab[p, 0:OBS, :] = next_ref[:, p * BATCH : (p + 1) * BATCH]
        tab[p, OBS : OBS + 1, :] = action_ref[:, p * BATCH : (p + 1) * BATCH]
        tab[p, OBS + 1 :, :] = jnp.zeros((TAB - OBS - 1, BATCH), jnp.int32)
        for t in range(1, STEPS):
            @pl.when(p > plane)
            def _():
                nbuf[t, p * BATCH : (p + 1) * BATCH, :] = jnp.zeros((BATCH, W), jnp.float32)
    idx[pl.ds(sec, 1)] = tab[pl.ds(plane, 1)]

    pl.semaphore_wait(barrier, SECTIONS - 1 + SHARDS - 1 + 2 * PLANES)

    def idx_copy(d):
        to = other_section(d)
        return pltpu.make_async_remote_copy(
            src_ref=tab.at[lax.rem(to, PLANES)], dst_ref=idx.at[sec],
            send_sem=idx_ssem.at[d], recv_sem=idx_rsem.at[sec],
            device_id={"section": to, "state": st}, device_id_type=MESH,
        )

    @pl.when(sec == SECTIONS - 1)
    def _():
        for d in range(1, SECTIONS):
            idx_copy(d).start()

    reward_copy = pltpu.make_async_remote_copy(
        src_ref=reward_ref, dst_ref=reward, send_sem=reward_ssem, recv_sem=reward_rsem,
        device_id=z_neighbour(True, 0), device_id_type=MESH,
    )
    reward_copy.start()

    def prepare(t):
        h = STEPS - 1 - t

        @pl.when(h != sec)
        def _():
            pltpu.make_async_remote_copy(
                src_ref=idx.at[h], dst_ref=idx.at[h], send_sem=idx_ssem.at[0], recv_sem=idx_rsem.at[h],
                device_id={"section": sec, "state": other_state(1)}, device_id_type=MESH,
            ).wait_recv()

        turned[...] = idx[h].T
        table = turned[pl.ds(pl.multiple_of(half * ROWS, ROWS), ROWS), :]
        act = table[:, OBS : OBS + 1]
        row = jnp.zeros((ROWS, W), jnp.float32)
        for a in range(ACTIONS):
            row = jnp.where(act == a, reward[a : a + 1, :], row)
        rewrow[lax.rem(t, 2)] = row
        wide = jnp.broadcast_to(act, (ROWS, W))
        column = lax.broadcasted_iota(jnp.int32, (ROWS, BELIEFS), 1)
        for o in range(OBS):
            pick = table[:, o : o + 1]
            onehot[o * ROWS : (o + 1) * ROWS, :] = (
                jnp.where(column == pick, 1.0, 0.0).astype(jnp.bfloat16)
            )
            w = jnp.zeros((ROWS, W), jnp.float32)
            for a in range(ACTIONS):
                w = jnp.where(wide == a, obs[a, o : o + 1, :], w)
            weight[o] = w

    order = ((1, 2), (0, 2), (1, 1), (1, 3), (0, 1), (0, 3), (1, 0), (0, 0))

    def chip_at(k, flip):
        return lax.rem(lo + order[k][0] + flip, 2) * 4 + lax.rem(y + order[k][1], 4)

    def pair_copy(k, t):
        return pltpu.make_async_remote_copy(
            src_ref=pair_send.at[k], dst_ref=pair_recv.at[t, k],
            send_sem=pair_ssem.at[k], recv_sem=pair_rsem.at[t, k],
            device_id={"section": sec, "state": chip * 2 + 1 - core}, device_id_type=MESH,
        )

    def part_copy(k, t):
        return pltpu.make_async_remote_copy(
            src_ref=part_send.at[k], dst_ref=part_recv.at[t, k],
            send_sem=part_ssem.at[k], recv_sem=part_rsem.at[t, k],
            device_id={"section": sec, "state": chip_at(k, 0) * 2 + core}, device_id_type=MESH,
        )

    users = tuple((d, up) for d in range(PLANES) for up in (True, False))

    def row_copy(u, t):
        d, up = users[u]
        return pltpu.make_async_remote_copy(
            src_ref=fresh.at[t], dst_ref=nbuf.at[t + 1, rows_of(mine)],
            send_sem=row_ssem.at[u], recv_sem=row_rsem.at[t, mine],
            device_id=z_neighbour(up, d), device_id_type=MESH,
        )

    def feeds(u, t):
        return (plane + users[u][0] < PLANES) & (t < STEPS - 1)

    def out_copy(t):
        return pltpu.make_async_remote_copy(
            src_ref=fresh.at[t], dst_ref=final.at[rows_of(mine)],
            send_sem=out_ssem, recv_sem=out_rsem.at[mine],
            device_id={"section": STEPS - 1 - t, "state": ((1 - lo) * 4 + y) * 2 + core},
            device_id_type=MESH,
        )

    def goes_out(t):
        return (lax.rem(STEPS - 1 - t, PLANES) < plane) | (t == STEPS - 1)

    def wait_into(dst, sem):
        pltpu.make_async_remote_copy(
            src_ref=fresh.at[0], dst_ref=dst, send_sem=out_ssem, recv_sem=sem,
            device_id=z_neighbour(True, 0), device_id_type=MESH,
        ).wait_recv()

    def wait_sent(t):
        for u in range(len(users)):
            @pl.when(feeds(u, t))
            def _():
                row_copy(u, t).wait_send()

        @pl.when(goes_out(t))
        def _():
            out_copy(t).wait_send()

    loads[0].wait()
    reward_copy.wait_recv()
    prepare(0)

    @pl.when(sec < SECTIONS - 1)
    def _():
        for d in range(1, SECTIONS):
            idx_copy(d).start()

    loads[1].wait()
    loads[2].wait()

    def step(t, carry):
        following = nbuf[t]
        high = following.astype(jnp.bfloat16)
        low = (following - high.astype(jnp.float32)).astype(jnp.bfloat16)
        both = jnp.concatenate([high, low], axis=1)
        total = jnp.zeros((ROWS, W), jnp.float32)
        for c in range(OBS // GROUP):
            got = jnp.dot(
                onehot[c * GROUP * ROWS : (c + 1) * GROUP * ROWS, :], both,
                preferred_element_type=jnp.float32,
            )
            got = (got[:, :W] + got[:, W:]).reshape(GROUP, ROWS, W)
            total = total + jnp.sum(got * weight[c * GROUP : (c + 1) * GROUP], axis=0)
        act = turned[pl.ds(pl.multiple_of(half * ROWS, ROWS), ROWS), :][:, OBS : OBS + 1]
        for a in range(ACTIONS):
            masked[:, a * W : (a + 1) * W] = jnp.where(act == a, total, 0.0).astype(jnp.bfloat16)

        for k in range(CHIPS):
            part = jnp.dot(
                masked[...], trans[:, pl.ds(pl.multiple_of(chip_at(k, 1) * 2 * W, 2 * W), 2 * W)],
                preferred_element_type=jnp.float32,
            )
            pair_send[k] = jnp.where(core == 0, part[:, W:], part[:, :W])
            pair_copy(k, t).start()
            part_send[k] = jnp.where(core == 0, part[:, :W], part[:, W:])
        for k in range(CHIPS):
            pair_copy(k, t).wait_recv()
            part_send[k] = part_send[k] + pair_recv[t, k]
            if k < CHIPS - 1:
                part_copy(k, t).start()

        @pl.when(t > 0)
        def _():
            wait_sent(t - 1)

        @pl.when(t < STEPS - 1)
        def _():
            prepare(t + 1)

        for k in range(CHIPS):
            pair_copy(k, t).wait_send()
        summed = part_send[CHIPS - 1]
        for k in range(CHIPS - 1):
            part_copy(k, t).wait_recv()
            summed = summed + part_recv[t, k]
        fresh[t] = rewrow[lax.rem(t, 2)] + discount * summed
        for u in range(len(users)):
            @pl.when(feeds(u, t))
            def _():
                row_copy(u, t).start()

        @pl.when(goes_out(t))
        def _():
            out_copy(t).start()

        for k in range(CHIPS - 1):
            part_copy(k, t).wait_send()

        @pl.when(t < STEPS - 1)
        def _():
            for m in range(2 * PLANES):
                @pl.when(m // 2 <= plane)
                def _():
                    wait_into(nbuf.at[t + 1, rows_of(m)], row_rsem.at[t, m])

        return carry

    lax.fori_loop(0, STEPS, step, 0)

    own = STEPS - 1 - sec
    loads[3].wait()
    for p in range(PLANES):
        used = (p <= plane) & (sec > 0)

        @pl.when(used)
        def _():
            final[p * BATCH : (p + 1) * BATCH, :] = nbuf[own + 1, p * BATCH : (p + 1) * BATCH, :]

        @pl.when(jnp.logical_not(used))
        def _():
            for m in (2 * p, 2 * p + 1):
                wait_into(final.at[rows_of(m)], out_rsem.at[m])

        block = final[p * BATCH : (p + 1) * BATCH, :] * belief[p * BATCH : (p + 1) * BATCH, :]
        vbuf[pl.ds(st, 1), p : p + 1, :] = jnp.sum(block.T, axis=0, keepdims=True)[None]

    def val_copy(d):
        return pltpu.make_async_remote_copy(
            src_ref=vbuf.at[st], dst_ref=vbuf.at[st],
            send_sem=val_ssem.at[d], recv_sem=val_rsem.at[d],
            device_id={"section": sec, "state": other_state(d)}, device_id_type=MESH,
        )

    for d in range(1, SHARDS):
        val_copy(d).start()
    wait_sent(STEPS - 1)
    reward_copy.wait_send()
    for d in range(1, SECTIONS):
        idx_copy(d).wait_send()
    for d in range(1, SHARDS):
        val_copy(d).wait_recv()
    for d in range(1, SHARDS):
        val_copy(d).wait_send()


def finish(final_ref, vbuf_ref, alphas_ref, values_ref):
    alphas_ref[...] = final_ref[...]
    value = vbuf_ref[0]
    for s in range(1, SHARDS):
        value = value + vbuf_ref[s]
    values_ref[...] = value


def local(belief, action, next_index, obs_table, transition, reward, terminal):
    vmem = pl.BlockSpec(memory_space=pltpu.VMEM)
    anywhere = pl.BlockSpec(memory_space=pl.ANY)
    dma = pltpu.SemaphoreType.DMA
    f32 = jnp.float32
    final, parts = pl.pallas_call(
        kernel,
        out_shape=(
            jax.ShapeDtypeStruct((BELIEFS, W), f32),
            jax.ShapeDtypeStruct((SHARDS, PLANES, W), f32),
        ),
        in_specs=[vmem, vmem, vmem, anywhere, anywhere, anywhere, anywhere],
        out_specs=(vmem, vmem),
        scratch_shapes=[
            pltpu.VMEM((ACTIONS, OBS, W), f32),
            pltpu.VMEM((ACTIONS * W, SHARDS * W), jnp.bfloat16),
            pltpu.VMEM((BELIEFS, W), f32),
            pltpu.VMEM((STEPS + 1, BELIEFS, W), f32),
            pltpu.VMEM((PLANES, TAB, BATCH), jnp.int32),
            pltpu.VMEM((SECTIONS, TAB, BATCH), jnp.int32),
            pltpu.VMEM((BATCH, TAB), jnp.int32),
            pltpu.VMEM((OBS * ROWS, BELIEFS), jnp.bfloat16),
            pltpu.VMEM((OBS, ROWS, W), f32),
            pltpu.VMEM((ACTIONS, W), f32),
            pltpu.VMEM((2, ROWS, W), f32),
            pltpu.VMEM((ROWS, ACTIONS * W), jnp.bfloat16),
            pltpu.VMEM((CHIPS, ROWS, W), f32),
            pltpu.VMEM((STEPS, CHIPS, ROWS, W), f32),
            pltpu.VMEM((CHIPS, ROWS, W), f32),
            pltpu.VMEM((STEPS, CHIPS, ROWS, W), f32),
            pltpu.VMEM((STEPS, ROWS, W), f32),
            dma((4,)),
            dma((SECTIONS,)),
            dma((SECTIONS,)),
            dma,
            dma,
            dma((CHIPS,)),
            dma((STEPS, CHIPS)),
            dma((CHIPS,)),
            dma((STEPS, CHIPS)),
            dma((2 * PLANES,)),
            dma((STEPS, 2 * PLANES)),
            dma,
            dma((2 * PLANES,)),
            dma((SHARDS,)),
            dma((SHARDS,)),
        ],
        compiler_params=pltpu.CompilerParams(
            collective_id=0, has_side_effects=True, vmem_limit_bytes=60 * 1024 * 1024
        ),
        name="chain",
    )(
        next_index[0].T, action, reward, obs_table, terminal,
        transition.reshape(ACTIONS * W, SHARDS * W), belief[0],
    )
    alphas, values = pl.pallas_call(
        finish,
        out_shape=(
            jax.ShapeDtypeStruct((BELIEFS, W), f32),
            jax.ShapeDtypeStruct((PLANES, W), f32),
        ),
        in_specs=[vmem, vmem],
        out_specs=(vmem, vmem),
        name="finish",
    )(final, parts)
    return alphas[None], values.reshape(1, BELIEFS)


def solution(mesh):
    return jax.shard_map(
        local,
        mesh=mesh,
        in_specs=(
            P("section", None, "state"),
            P("section", None),
            P("section", None, None),
            P(None, None, "state"),
            P(None, "state", None),
            P(None, "state"),
            P(None, "state"),
        ),
        out_specs=(P("section", None, "state"), P("section", None)),
        check_vma=False,
    )
```

```python
import jax
import jax.numpy as jnp
from jax import lax
from jax.experimental import pallas as pl
from jax.experimental.pallas import tpu as pltpu
from jax.sharding import PartitionSpec as P

MESH = pl.DeviceIdType.MESH
discount = 0.95

ACTIONS = 8
OBS = 32
STEPS = 8
SECTIONS = 8
PLANES = 4
CHIPS = 8
SHARDS = 16
BELIEFS = 512
BATCH = 128
ROWS = 64
W = 128
FOLD = 256
TAB = 40
GROUP = 8


def kernel(
    next_ref, action_ref, reward_ref, obs_hbm, terminal_hbm, trans_hbm, belief_hbm,
    final, vbuf,
    obs, trans, belief, nbuf, tab, idx, turned, onehot, weight, rewrow, masked,
    pair_send, pair_recv, part_send, part_recv,
    load_sem, idx_ssem, idx_rsem, pair_ssem, pair_rsem, part_ssem, part_rsem,
    row_ssem, row_rsem, out_ssem, out_rsem, val_ssem, val_rsem,
):
    sec = lax.axis_index("section")
    st = lax.axis_index("state")
    plane, half = lax.rem(sec, PLANES), lax.div(sec, PLANES)
    core, chip = lax.rem(st, 2), lax.div(st, 2)
    lo, y = lax.div(chip, 4), lax.rem(chip, 4)

    def rows_of(p, q):
        return pl.ds(pl.multiple_of((p * 2 + q) * ROWS, ROWS), ROWS)

    def other_section(d):
        return lax.rem(sec + d, SECTIONS)

    def other_state(d):
        return lax.rem(st + d, SHARDS)

    def other_plane(d):
        return lax.rem(plane + d, PLANES)

    def z_neighbour(up, dy):
        z = lax.rem(half * 2 + lo + (1 if up else 3), 4)
        return {
            "section": lax.div(z, 2) * PLANES + plane,
            "state": (lax.rem(z, 2) * 4 + lax.rem(y + dy, 4)) * 2 + core,
        }

    loads = [
        pltpu.make_async_copy(obs_hbm, obs, load_sem.at[0]),
        pltpu.make_async_copy(terminal_hbm, nbuf.at[0], load_sem.at[1]),
        pltpu.make_async_copy(trans_hbm, trans, load_sem.at[2]),
        pltpu.make_async_copy(belief_hbm, belief, load_sem.at[3]),
    ]
    for load in loads:
        load.start()

    barrier = pltpu.get_barrier_semaphore()
    for d in range(1, SECTIONS):
        pl.semaphore_signal(barrier, inc=1, device_id={"section": other_section(d), "state": st}, device_id_type=MESH)
    for d in range(1, SHARDS):
        pl.semaphore_signal(barrier, inc=1, device_id={"section": sec, "state": other_state(d)}, device_id_type=MESH)
    for up in (True, False):
        for dy in range(4):
            pl.semaphore_signal(barrier, inc=1, device_id=z_neighbour(up, dy), device_id_type=MESH)

    for p in range(PLANES):
        tab[p, 0:OBS, :] = next_ref[:, p * BATCH : (p + 1) * BATCH]
        tab[p, OBS : OBS + 1, :] = action_ref[:, p * BATCH : (p + 1) * BATCH]
        tab[p, OBS + 1 :, :] = jnp.zeros((TAB - OBS - 1, BATCH), jnp.int32)
        for t in range(1, STEPS):
            @pl.when(p > plane)
            def _():
                nbuf[t, p * BATCH : (p + 1) * BATCH, :] = jnp.zeros((BATCH, W), jnp.float32)
    idx[pl.ds(sec, 1)] = tab[pl.ds(plane, 1)]

    pl.semaphore_wait(barrier, SECTIONS - 1 + SHARDS - 1 + 8)

    def idx_copy(d):
        to = other_section(d)
        return pltpu.make_async_remote_copy(
            src_ref=tab.at[lax.rem(to, PLANES)], dst_ref=idx.at[sec],
            send_sem=idx_ssem.at[d], recv_sem=idx_rsem.at[sec],
            device_id={"section": to, "state": st}, device_id_type=MESH,
        )

    @pl.when(sec == SECTIONS - 1)
    def _():
        for d in range(1, SECTIONS):
            idx_copy(d).start()

    def prepare(t):
        h = STEPS - 1 - t

        @pl.when(h != sec)
        def _():
            pltpu.make_async_remote_copy(
                src_ref=idx.at[h], dst_ref=idx.at[h], send_sem=idx_ssem.at[0], recv_sem=idx_rsem.at[h],
                device_id={"section": sec, "state": other_state(1)}, device_id_type=MESH,
            ).wait_recv()

        turned[...] = idx[h].T
        act = turned[:, OBS : OBS + 1]
        row = jnp.zeros((BATCH, W), jnp.float32)
        for a in range(ACTIONS):
            row = jnp.where(act == a, reward_ref[a : a + 1, :], row)
        rewrow[lax.rem(t, 2)] = row
        wide = jnp.broadcast_to(act, (BATCH, W))
        column = lax.broadcasted_iota(jnp.int32, (BATCH, FOLD), 1)
        for o in range(OBS):
            pick = turned[:, o : o + 1]
            hit = jnp.where(column == lax.rem(pick, FOLD), 1.0, 0.0).astype(jnp.bfloat16)
            w = jnp.zeros((BATCH, W), jnp.float32)
            for a in range(ACTIONS):
                w = jnp.where(wide == a, obs[a, o : o + 1, :], w)
            upper = jnp.broadcast_to(pick >= FOLD, (BATCH, W))
            w_low, w_up = jnp.where(upper, 0.0, w), jnp.where(upper, w, 0.0)
            for q in (0, 1):
                onehot[q, o * ROWS : (o + 1) * ROWS, :] = hit[q * ROWS : (q + 1) * ROWS, :]
                weight[q, o, :, :W] = w_low[q * ROWS : (q + 1) * ROWS, :]
                weight[q, o, :, W:] = w_up[q * ROWS : (q + 1) * ROWS, :]

    order = ((1, 2), (0, 2), (1, 1), (1, 3), (0, 1), (0, 3), (1, 0), (0, 0))

    def block_at(k):
        return lax.rem(lo + order[k][0], 2) * 4 + lax.rem(y + order[k][1], 4)

    def user_of(q, k):
        if order[k][0]:
            return z_neighbour(q == 0, order[k][1])
        return {"section": sec, "state": block_at(k) * 2 + core}

    def pair_copy(q, k, t):
        return pltpu.make_async_remote_copy(
            src_ref=pair_send.at[q, k], dst_ref=pair_recv.at[t, q, k],
            send_sem=pair_ssem.at[q, k], recv_sem=pair_rsem.at[t, q, k],
            device_id={"section": sec, "state": chip * 2 + 1 - core}, device_id_type=MESH,
        )

    def part_copy(q, k, t):
        return pltpu.make_async_remote_copy(
            src_ref=part_send.at[q, k], dst_ref=part_recv.at[t, q, k],
            send_sem=part_ssem.at[q, k], recv_sem=part_rsem.at[t, q, k],
            device_id=user_of(q, k), device_id_type=MESH,
        )

    def row_copy(q, d, t):
        return pltpu.make_async_remote_copy(
            src_ref=nbuf.at[t + 1, rows_of(plane, q)], dst_ref=nbuf.at[t + 1, rows_of(plane, q)],
            send_sem=row_ssem.at[q, d], recv_sem=row_rsem.at[t, plane, q],
            device_id={"section": half * PLANES + other_plane(d), "state": st}, device_id_type=MESH,
        )

    def feeds(d, t):
        return (plane + d < PLANES) & (t < STEPS - 1)

    def out_copy(q, t):
        return pltpu.make_async_remote_copy(
            src_ref=nbuf.at[t + 1, rows_of(plane, q)], dst_ref=final.at[rows_of(plane, q)],
            send_sem=out_ssem.at[q], recv_sem=out_rsem.at[plane, q],
            device_id={"section": STEPS - 1 - t, "state": st}, device_id_type=MESH,
        )

    def goes_out(t):
        owner = STEPS - 1 - t
        return (lax.div(owner, PLANES) == half) & (lax.rem(owner, PLANES) < plane)

    def wait_into(dst, sem):
        pltpu.make_async_remote_copy(
            src_ref=pair_send.at[0, 0], dst_ref=dst, send_sem=out_ssem.at[0], recv_sem=sem,
            device_id={"section": half * PLANES + other_plane(1), "state": st}, device_id_type=MESH,
        ).wait_recv()

    def wait_sent(t):
        for q in (0, 1):
            for d in range(1, PLANES):
                @pl.when(feeds(d, t))
                def _():
                    row_copy(q, d, t).wait_send()

            @pl.when(goes_out(t))
            def _():
                out_copy(q, t).wait_send()

    loads[0].wait()
    prepare(0)

    @pl.when(sec < SECTIONS - 1)
    def _():
        for d in range(1, SECTIONS):
            idx_copy(d).start()

    loads[1].wait()
    loads[2].wait()

    def gather(q, folded):
        total = jnp.zeros((ROWS, 2 * W), jnp.float32)
        for c in range(OBS // GROUP):
            got = jnp.dot(
                onehot[q, c * GROUP * ROWS : (c + 1) * GROUP * ROWS, :], folded,
                preferred_element_type=jnp.float32,
            ).reshape(GROUP, ROWS, 2 * W)
            total = total + jnp.sum(got * weight[q, c * GROUP : (c + 1) * GROUP], axis=0)
        total = total[:, :W] + total[:, W:]
        act = turned[q * ROWS : (q + 1) * ROWS, OBS : OBS + 1]
        for a in range(ACTIONS):
            masked[q, :, a * W : (a + 1) * W] = jnp.where(act == a, total, 0.0).astype(jnp.bfloat16)

    def multiply(q, t):
        for k in range(CHIPS):
            part = jnp.dot(
                masked[q], trans[:, pl.ds(pl.multiple_of(block_at(k) * 2 * W, 2 * W), 2 * W)],
                preferred_element_type=jnp.float32,
            )
            pair_send[q, k] = jnp.where(core == 0, part[:, W:], part[:, :W])
            pair_copy(q, k, t).start()
            part_send[q, k] = jnp.where(core == 0, part[:, :W], part[:, W:])

    def send_parts(q, t):
        for k in range(CHIPS):
            pair_copy(q, k, t).wait_recv()
            part_send[q, k] = part_send[q, k] + pair_recv[t, q, k]
            if k < CHIPS - 1:
                part_copy(q, k, t).start()

    def add_parts(q, t):
        summed = part_send[q, CHIPS - 1]
        for k in range(CHIPS - 1):
            part_copy(q, k, t).wait_recv()
            summed = summed + part_recv[t, q, k]
        nbuf[t + 1, rows_of(plane, q)] = (
            rewrow[lax.rem(t, 2), q * ROWS : (q + 1) * ROWS, :] + discount * summed
        )
        for d in range(1, PLANES):
            @pl.when(feeds(d, t))
            def _():
                row_copy(q, d, t).start()

        @pl.when(goes_out(t))
        def _():
            out_copy(q, t).start()

    def step(t, carry):
        following = nbuf[t].astype(jnp.bfloat16)
        folded = jnp.concatenate([following[:FOLD], following[FOLD:]], axis=1)
        gather(0, folded)
        multiply(0, t)
        gather(1, folded)
        send_parts(0, t)
        multiply(1, t)
        send_parts(1, t)

        @pl.when(t > 0)
        def _():
            wait_sent(t - 1)

        @pl.when(t < STEPS - 1)
        def _():
            prepare(t + 1)

        for q in (0, 1):
            for k in range(CHIPS):
                pair_copy(q, k, t).wait_send()
        for q in (0, 1):
            add_parts(q, t)
            for k in range(CHIPS - 1):
                part_copy(q, k, t).wait_send()

        @pl.when(t < STEPS - 1)
        def _():
            for p in range(PLANES - 1):
                @pl.when(p < plane)
                def _():
                    for q in (0, 1):
                        wait_into(nbuf.at[t + 1, rows_of(p, q)], row_rsem.at[t, p, q])

        return carry

    lax.fori_loop(0, STEPS, step, 0)

    own = STEPS - 1 - sec
    for p in range(PLANES):
        @pl.when(p <= plane)
        def _():
            final[p * BATCH : (p + 1) * BATCH, :] = nbuf[own + 1, p * BATCH : (p + 1) * BATCH, :]

    loads[3].wait()
    for p in range(PLANES):
        @pl.when(p > plane)
        def _():
            for q in (0, 1):
                wait_into(final.at[rows_of(p, q)], out_rsem.at[p, q])

        block = final[p * BATCH : (p + 1) * BATCH, :] * belief[p * BATCH : (p + 1) * BATCH, :]
        vbuf[pl.ds(st, 1), p : p + 1, :] = jnp.sum(block.T, axis=0, keepdims=True)[None]

    def val_copy(d):
        return pltpu.make_async_remote_copy(
            src_ref=vbuf.at[st], dst_ref=vbuf.at[st],
            send_sem=val_ssem.at[d], recv_sem=val_rsem.at[d],
            device_id={"section": sec, "state": other_state(d)}, device_id_type=MESH,
        )

    for d in range(1, SHARDS):
        val_copy(d).start()
    wait_sent(STEPS - 1)
    for d in range(1, SECTIONS):
        idx_copy(d).wait_send()
    for d in range(1, SHARDS):
        val_copy(d).wait_recv()
    for d in range(1, SHARDS):
        val_copy(d).wait_send()


def finish(final_ref, vbuf_ref, alphas_ref, values_ref):
    alphas_ref[...] = final_ref[...]
    value = vbuf_ref[0]
    for s in range(1, SHARDS):
        value = value + vbuf_ref[s]
    values_ref[...] = value


def local(belief, action, next_index, obs_table, transition, reward, terminal):
    vmem = pl.BlockSpec(memory_space=pltpu.VMEM)
    anywhere = pl.BlockSpec(memory_space=pl.ANY)
    dma = pltpu.SemaphoreType.DMA
    f32 = jnp.float32
    final, parts = pl.pallas_call(
        kernel,
        out_shape=(
            jax.ShapeDtypeStruct((BELIEFS, W), f32),
            jax.ShapeDtypeStruct((SHARDS, PLANES, W), f32),
        ),
        in_specs=[vmem, vmem, vmem, anywhere, anywhere, anywhere, anywhere],
        out_specs=(vmem, vmem),
        scratch_shapes=[
            pltpu.VMEM((ACTIONS, OBS, W), f32),
            pltpu.VMEM((ACTIONS * W, SHARDS * W), jnp.bfloat16),
            pltpu.VMEM((BELIEFS, W), f32),
            pltpu.VMEM((STEPS + 1, BELIEFS, W), f32),
            pltpu.VMEM((PLANES, TAB, BATCH), jnp.int32),
            pltpu.VMEM((SECTIONS, TAB, BATCH), jnp.int32),
            pltpu.VMEM((BATCH, TAB), jnp.int32),
            pltpu.VMEM((2, OBS * ROWS, FOLD), jnp.bfloat16),
            pltpu.VMEM((2, OBS, ROWS, 2 * W), f32),
            pltpu.VMEM((2, BATCH, W), f32),
            pltpu.VMEM((2, ROWS, ACTIONS * W), jnp.bfloat16),
            pltpu.VMEM((2, CHIPS, ROWS, W), f32),
            pltpu.VMEM((STEPS, 2, CHIPS, ROWS, W), f32),
            pltpu.VMEM((2, CHIPS, ROWS, W), f32),
            pltpu.VMEM((STEPS, 2, CHIPS, ROWS, W), f32),
            dma((4,)),
            dma((SECTIONS,)),
            dma((SECTIONS,)),
            dma((2, CHIPS)),
            dma((STEPS, 2, CHIPS)),
            dma((2, CHIPS)),
            dma((STEPS, 2, CHIPS)),
            dma((2, PLANES)),
            dma((STEPS, PLANES, 2)),
            dma((2,)),
            dma((PLANES, 2)),
            dma((SHARDS,)),
            dma((SHARDS,)),
        ],
        compiler_params=pltpu.CompilerParams(
            collective_id=0, has_side_effects=True, vmem_limit_bytes=60 * 1024 * 1024
        ),
        name="chain",
    )(
        next_index[0].T, action, reward, obs_table, terminal,
        transition.reshape(ACTIONS * W, SHARDS * W), belief[0],
    )
    alphas, values = pl.pallas_call(
        finish,
        out_shape=(
            jax.ShapeDtypeStruct((BELIEFS, W), f32),
            jax.ShapeDtypeStruct((PLANES, W), f32),
        ),
        in_specs=[vmem, vmem],
        out_specs=(vmem, vmem),
        name="finish",
    )(final, parts)
    return alphas[None], values.reshape(1, BELIEFS)


def solution(mesh):
    return jax.shard_map(
        local,
        mesh=mesh,
        in_specs=(
            P("section", None, "state"),
            P("section", None),
            P("section", None, None),
            P(None, None, "state"),
            P(None, "state", None),
            P(None, "state"),
            P(None, "state"),
        ),
        out_specs=(P("section", None, "state"), P("section", None)),
        check_vma=False,
    )
```

```python
import jax
import jax.numpy as jnp
from jax import lax
from jax.experimental import pallas as pl
from jax.experimental.pallas import tpu as pltpu
from jax.sharding import PartitionSpec as P

MESH = pl.DeviceIdType.MESH
discount = 0.95

ACTIONS = 8
OBS = 32
STEPS = 8
SECTIONS = 8
PLANES = 4
CHIPS = 8
SHARDS = 16
BELIEFS = 512
BATCH = 128
ROWS = 64
W = 128
FOLD = 256
TAB = 40
GROUP = 8
GROUPS = ((0,), (1, 2), (3, 4), (5, 6, 7))
LAST = STEPS - 1


def kernel(
    next_ref, action_ref, reward_ref, obs_hbm, terminal_hbm, trans_hbm, belief_hbm,
    final, vbuf,
    obs, trans, belief, nbuf, tab, idx, turned, onehot, weight, reward, rewrow, masked,
    pair_send, pair_recv, part_send, part_recv, fresh,
    bel, vsend, own_ssem, own_rsem, load_sem, bel_ssem, bel_rsem, idx_ssem, idx_rsem, reward_ssem, reward_rsem, pair_ssem, pair_rsem, part_ssem, part_rsem,
    row_ssem, row_rsem, out_ssem, out_rsem, val_ssem, val_rsem,
):
    sec = lax.axis_index("section")
    st = lax.axis_index("state")
    plane, half = lax.rem(sec, PLANES), lax.div(sec, PLANES)
    core, chip = lax.rem(st, 2), lax.div(st, 2)
    lo, y = lax.div(chip, 4), lax.rem(chip, 4)

    mine = plane * 2 + half

    def rows_of(m):
        return pl.ds(pl.multiple_of(m * ROWS, ROWS), ROWS)

    def other_section(d):
        return lax.rem(sec + d, SECTIONS)

    def other_state(d):
        return lax.rem(st + d, SHARDS)

    def z_neighbour(up, d):
        z = lax.rem(half * 2 + lo + (1 if up else 3), 4)
        return {
            "section": lax.div(z, 2) * PLANES + lax.rem(plane + d, PLANES),
            "state": (lax.rem(z, 2) * 4 + y) * 2 + core,
        }

    loads = [
        pltpu.make_async_copy(obs_hbm, obs, load_sem.at[0]),
        pltpu.make_async_copy(terminal_hbm, nbuf.at[0], load_sem.at[1]),
        pltpu.make_async_copy(trans_hbm, trans, load_sem.at[2]),
        pltpu.make_async_copy(belief_hbm, belief, load_sem.at[3]),
    ]
    for load in loads:
        load.start()

    barrier = pltpu.get_barrier_semaphore()
    for d in range(1, SECTIONS):
        pl.semaphore_signal(barrier, inc=1, device_id={"section": other_section(d), "state": st}, device_id_type=MESH)
    for d in range(1, SHARDS):
        pl.semaphore_signal(barrier, inc=1, device_id={"section": sec, "state": other_state(d)}, device_id_type=MESH)
    for up in (True, False):
        for d in range(PLANES):
            pl.semaphore_signal(barrier, inc=1, device_id=z_neighbour(up, d), device_id_type=MESH)

    for p in range(PLANES):
        tab[p, 0:OBS, :] = next_ref[:, p * BATCH : (p + 1) * BATCH]
        tab[p, OBS : OBS + 1, :] = action_ref[:, p * BATCH : (p + 1) * BATCH]
        tab[p, OBS + 1 :, :] = jnp.zeros((TAB - OBS - 1, BATCH), jnp.int32)
        for t in range(1, STEPS):
            @pl.when(p > plane)
            def _():
                nbuf[t, p * BATCH : (p + 1) * BATCH, :] = jnp.zeros((BATCH, W), jnp.float32)
    idx[pl.ds(sec, 1)] = tab[pl.ds(plane, 1)]

    pl.semaphore_wait(barrier, SECTIONS - 1 + SHARDS - 1 + 2 * PLANES)

    def idx_copy(d):
        to = other_section(d)
        return pltpu.make_async_remote_copy(
            src_ref=tab.at[lax.rem(to, PLANES)], dst_ref=idx.at[sec],
            send_sem=idx_ssem.at[d], recv_sem=idx_rsem.at[sec],
            device_id={"section": to, "state": st}, device_id_type=MESH,
        )

    @pl.when(sec == SECTIONS - 1)
    def _():
        for d in (1, 5, 2, 6, 3, 7, 4):
            idx_copy(d).start()

    reward_copy = pltpu.make_async_remote_copy(
        src_ref=reward_ref, dst_ref=reward, send_sem=reward_ssem, recv_sem=reward_rsem,
        device_id=z_neighbour(True, 0), device_id_type=MESH,
    )
    reward_copy.start()

    def prepare(t):
        h = STEPS - 1 - t

        @pl.when(h != sec)
        def _():
            pltpu.make_async_remote_copy(
                src_ref=idx.at[h], dst_ref=idx.at[h], send_sem=idx_ssem.at[0], recv_sem=idx_rsem.at[h],
                device_id={"section": sec, "state": other_state(1)}, device_id_type=MESH,
            ).wait_recv()

        turned[...] = idx[h].T
        table = turned[pl.ds(pl.multiple_of(half * ROWS, ROWS), ROWS), :]
        act = table[:, OBS : OBS + 1]
        row = jnp.zeros((ROWS, W), jnp.float32)
        for a in range(ACTIONS):
            row = jnp.where(act == a, reward[a : a + 1, :], row)
        rewrow[lax.rem(t, 2)] = row
        wide = jnp.broadcast_to(act, (ROWS, W))
        column = lax.broadcasted_iota(jnp.int32, (ROWS, FOLD), 1)
        for o in range(OBS):
            pick = table[:, o : o + 1]
            onehot[o * ROWS : (o + 1) * ROWS, :] = (
                jnp.where(column == lax.rem(pick, FOLD), 1.0, 0.0).astype(jnp.bfloat16)
            )
            w = jnp.zeros((ROWS, W), jnp.float32)
            for a in range(ACTIONS):
                w = jnp.where(wide == a, obs[a, o : o + 1, :], w)
            upper = jnp.broadcast_to(pick >= FOLD, (ROWS, W))
            weight[o, :, :W] = jnp.where(upper, 0.0, w)
            weight[o, :, W:] = jnp.where(upper, w, 0.0)

    order = ((1, 2), (0, 2), (1, 1), (1, 3), (0, 1), (0, 3), (1, 0), (0, 0))

    def chip_at(k, flip):
        return lax.rem(lo + order[k][0] + flip, 2) * 4 + lax.rem(y + order[k][1], 4)

    def pair_copy(k, t):
        return pltpu.make_async_remote_copy(
            src_ref=pair_send.at[k], dst_ref=pair_recv.at[t, k],
            send_sem=pair_ssem.at[k], recv_sem=pair_rsem.at[t, k],
            device_id={"section": sec, "state": chip * 2 + 1 - core}, device_id_type=MESH,
        )

    def part_copy(k, t):
        return pltpu.make_async_remote_copy(
            src_ref=part_send.at[k], dst_ref=part_recv.at[t, k],
            send_sem=part_ssem.at[k], recv_sem=part_rsem.at[t, k],
            device_id={"section": sec, "state": chip_at(k, 0) * 2 + core}, device_id_type=MESH,
        )

    users = tuple((d, up) for d in range(PLANES) for up in (True, False))

    def row_copy(u, t):
        d, up = users[u]
        return pltpu.make_async_remote_copy(
            src_ref=fresh.at[t], dst_ref=nbuf.at[t + 1, rows_of(mine)],
            send_sem=row_ssem.at[u], recv_sem=row_rsem.at[t, mine],
            device_id=z_neighbour(up, d), device_id_type=MESH,
        )

    def feeds(u, t):
        return (plane + users[u][0] < PLANES) & (t < STEPS - 1)

    def out_copy(t):
        return pltpu.make_async_remote_copy(
            src_ref=fresh.at[t], dst_ref=final.at[rows_of(mine)],
            send_sem=out_ssem, recv_sem=out_rsem.at[mine],
            device_id={"section": STEPS - 1 - t, "state": ((1 - lo) * 4 + y) * 2 + core},
            device_id_type=MESH,
        )

    def goes_out(t):
        return (lax.rem(STEPS - 1 - t, PLANES) < plane) | (t == STEPS - 1)

    def bel_copy(m):
        return pltpu.make_async_remote_copy(
            src_ref=belief.at[m * ROWS : (m + 1) * ROWS], dst_ref=bel,
            send_sem=bel_ssem.at[m], recv_sem=bel_rsem,
            device_id={"section": (m % 2) * PLANES + m // 2, "state": ((1 - lo) * 4 + y) * 2 + core},
            device_id_type=MESH,
        )

    def own_val_copy(s):
        return pltpu.make_async_remote_copy(
            src_ref=vsend, dst_ref=vbuf.at[st, pl.ds(mine, 1)], send_sem=own_ssem.at[s], recv_sem=own_rsem.at[mine],
            device_id={"section": 0, "state": s}, device_id_type=MESH,
        )

    def elsewhere(s):
        return (sec > 0) | (st != s)

    def wait_into(dst, sem):
        pltpu.make_async_remote_copy(
            src_ref=fresh.at[0], dst_ref=dst, send_sem=out_ssem, recv_sem=sem,
            device_id=z_neighbour(True, 0), device_id_type=MESH,
        ).wait_recv()

    def wait_sent(t):
        for u in range(len(users)):
            @pl.when(feeds(u, t))
            def _():
                row_copy(u, t).wait_send()

        @pl.when(goes_out(t))
        def _():
            out_copy(t).wait_send()

    loads[0].wait()
    reward_copy.wait_recv()
    prepare(0)

    @pl.when(sec < SECTIONS - 1)
    def _():
        for d in range(1, SECTIONS):
            idx_copy(d).start()

    loads[1].wait()
    loads[2].wait()

    def step(t, carry):
        following = nbuf[t].astype(jnp.bfloat16)
        folded = jnp.concatenate([following[:FOLD], following[FOLD:]], axis=1)
        total = jnp.zeros((ROWS, 2 * W), jnp.float32)
        for c in range(OBS // GROUP):
            got = jnp.dot(
                onehot[c * GROUP * ROWS : (c + 1) * GROUP * ROWS, :], folded,
                preferred_element_type=jnp.float32,
            ).reshape(GROUP, ROWS, 2 * W)
            total = total + jnp.sum(got * weight[c * GROUP : (c + 1) * GROUP], axis=0)
        total = total[:, :W] + total[:, W:]
        act = turned[pl.ds(pl.multiple_of(half * ROWS, ROWS), ROWS), :][:, OBS : OBS + 1]
        for a in range(ACTIONS):
            masked[:, a * W : (a + 1) * W] = jnp.where(act == a, total, 0.0).astype(jnp.bfloat16)

        for group in GROUPS:
            parts = [
                jnp.dot(
                    masked[...], trans[:, pl.ds(pl.multiple_of(chip_at(k, 1) * 2 * W, 2 * W), 2 * W)],
                    preferred_element_type=jnp.float32,
                )
                for k in group
            ]
            for k, part in zip(group, parts):
                pair_send[k] = jnp.where(core == 0, part[:, W:], part[:, :W])
                part_send[k] = jnp.where(core == 0, part[:, :W], part[:, W:])
            for k in group:
                pair_copy(k, t).start()
        for k in range(CHIPS):
            pair_copy(k, t).wait_recv()
            part_send[k] = part_send[k] + pair_recv[t, k]
            if k < CHIPS - 1:
                part_copy(k, t).start()

        @pl.when(t > 0)
        def _():
            wait_sent(t - 1)

        @pl.when(t < STEPS - 1)
        def _():
            prepare(t + 1)

        for k in range(CHIPS):
            pair_copy(k, t).wait_send()
        summed = part_send[CHIPS - 1]
        for k in range(CHIPS - 1):
            part_copy(k, t).wait_recv()
            summed = summed + part_recv[t, k]
        fresh[t] = rewrow[lax.rem(t, 2)] + discount * summed
        for u in range(len(users)):
            @pl.when(feeds(u, t))
            def _():
                row_copy(u, t).start()

        @pl.when(goes_out(t))
        def _():
            out_copy(t).start()

        @pl.when((t == LAST - 2) & (sec == 0))
        def _():
            loads[3].wait()
            for m in range(2 * PLANES):
                bel_copy(m).start()

        @pl.when(t == LAST)
        def _():
            bel_copy(0).wait_recv()
            product = fresh[t] * bel[...]
            nothing = jnp.zeros((ROWS, W), jnp.float32)
            first = jnp.concatenate([product, nothing], axis=0)
            second = jnp.concatenate([nothing, product], axis=0)
            both = jnp.where(half == 0, first, second)
            vsend[...] = jnp.sum(both.T, axis=0, keepdims=True)
            for s in range(SHARDS):
                @pl.when(elsewhere(s))
                def _():
                    own_val_copy(s).start()

        for k in range(CHIPS - 1):
            part_copy(k, t).wait_send()

        @pl.when(t < STEPS - 1)
        def _():
            for m in range(2 * PLANES):
                @pl.when(m // 2 <= plane)
                def _():
                    wait_into(nbuf.at[t + 1, rows_of(m)], row_rsem.at[t, m])

        return carry

    lax.fori_loop(0, STEPS, step, 0)

    own = STEPS - 1 - sec

    @pl.when(sec > 0)
    def _():
        loads[3].wait()

    for p in range(PLANES):
        used = (p <= plane) & (sec > 0)

        @pl.when(used)
        def _():
            final[p * BATCH : (p + 1) * BATCH, :] = nbuf[own + 1, p * BATCH : (p + 1) * BATCH, :]

        @pl.when(jnp.logical_not(used))
        def _():
            for m in (2 * p, 2 * p + 1):
                wait_into(final.at[rows_of(m)], out_rsem.at[m])

    def val_copy(d):
        return pltpu.make_async_remote_copy(
            src_ref=vbuf.at[st], dst_ref=vbuf.at[st],
            send_sem=val_ssem.at[d], recv_sem=val_rsem.at[d],
            device_id={"section": sec, "state": other_state(d)}, device_id_type=MESH,
        )

    @pl.when(sec > 0)
    def _():
        for p in range(PLANES):
            block = final[p * BATCH : (p + 1) * BATCH, :] * belief[p * BATCH : (p + 1) * BATCH, :]
            vbuf[pl.ds(st, 1), 2 * p : 2 * p + 1, :] = jnp.sum(block.T, axis=0, keepdims=True)[None]
            vbuf[pl.ds(st, 1), 2 * p + 1 : 2 * p + 2, :] = jnp.zeros((1, 1, W), jnp.float32)
        for d in range(1, SHARDS):
            val_copy(d).start()

    @pl.when(sec == 0)
    def _():
        vbuf[pl.ds(st, 1), 0:1, :] = vsend[...][None]
        for m in range(2 * PLANES):
            count = SHARDS if m else SHARDS - 1
            pltpu.make_async_remote_copy(
                src_ref=vbuf.at[pl.ds(0, count), m], dst_ref=vbuf.at[pl.ds(0, count), m],
                send_sem=own_ssem.at[0], recv_sem=own_rsem.at[m],
                device_id=z_neighbour(True, 0), device_id_type=MESH,
            ).wait_recv()

    wait_sent(STEPS - 1)
    reward_copy.wait_send()
    for d in range(1, SECTIONS):
        idx_copy(d).wait_send()
    for s in range(SHARDS):
        @pl.when(elsewhere(s))
        def _():
            own_val_copy(s).wait_send()

    @pl.when(sec == 0)
    def _():
        for m in range(2 * PLANES):
            bel_copy(m).wait_send()

    @pl.when(sec > 0)
    def _():
        for d in range(1, SHARDS):
            val_copy(d).wait_recv()
        for d in range(1, SHARDS):
            val_copy(d).wait_send()


def finish(final_ref, vbuf_ref, alphas_ref, values_ref):
    alphas_ref[...] = final_ref[...]
    value = vbuf_ref[0]
    for s in range(1, SHARDS):
        value = value + vbuf_ref[s]
    for p in range(PLANES):
        values_ref[p : p + 1, :] = value[2 * p : 2 * p + 1, :] + value[2 * p + 1 : 2 * p + 2, :]


def local(belief, action, next_index, obs_table, transition, reward, terminal):
    vmem = pl.BlockSpec(memory_space=pltpu.VMEM)
    anywhere = pl.BlockSpec(memory_space=pl.ANY)
    dma = pltpu.SemaphoreType.DMA
    f32 = jnp.float32
    final, parts = pl.pallas_call(
        kernel,
        out_shape=(
            jax.ShapeDtypeStruct((BELIEFS, W), f32),
            jax.ShapeDtypeStruct((SHARDS, 2 * PLANES, W), f32),
        ),
        in_specs=[vmem, vmem, vmem, anywhere, anywhere, anywhere, anywhere],
        out_specs=(vmem, vmem),
        scratch_shapes=[
            pltpu.VMEM((ACTIONS, OBS, W), f32),
            pltpu.VMEM((ACTIONS * W, SHARDS * W), jnp.bfloat16),
            pltpu.VMEM((BELIEFS, W), f32),
            pltpu.VMEM((STEPS + 1, BELIEFS, W), f32),
            pltpu.VMEM((PLANES, TAB, BATCH), jnp.int32),
            pltpu.VMEM((SECTIONS, TAB, BATCH), jnp.int32),
            pltpu.VMEM((BATCH, TAB), jnp.int32),
            pltpu.VMEM((OBS * ROWS, FOLD), jnp.bfloat16),
            pltpu.VMEM((OBS, ROWS, 2 * W), f32),
            pltpu.VMEM((ACTIONS, W), f32),
            pltpu.VMEM((2, ROWS, W), f32),
            pltpu.VMEM((ROWS, ACTIONS * W), jnp.bfloat16),
            pltpu.VMEM((CHIPS, ROWS, W), f32),
            pltpu.VMEM((STEPS, CHIPS, ROWS, W), f32),
            pltpu.VMEM((CHIPS, ROWS, W), f32),
            pltpu.VMEM((STEPS, CHIPS, ROWS, W), f32),
            pltpu.VMEM((STEPS, ROWS, W), f32),
            pltpu.VMEM((ROWS, W), f32),
            pltpu.VMEM((1, W), f32),
            dma((SHARDS,)),
            dma((2 * PLANES,)),
            dma((4,)),
            dma((2 * PLANES,)),
            dma,
            dma((SECTIONS,)),
            dma((SECTIONS,)),
            dma,
            dma,
            dma((CHIPS,)),
            dma((STEPS, CHIPS)),
            dma((CHIPS,)),
            dma((STEPS, CHIPS)),
            dma((2 * PLANES,)),
            dma((STEPS, 2 * PLANES)),
            dma,
            dma((2 * PLANES,)),
            dma((SHARDS,)),
            dma((SHARDS,)),
        ],
        compiler_params=pltpu.CompilerParams(
            collective_id=0, has_side_effects=True, vmem_limit_bytes=60 * 1024 * 1024
        ),
        name="chain",
    )(
        next_index[0].T, action, reward, obs_table, terminal,
        transition.reshape(ACTIONS * W, SHARDS * W), belief[0],
    )
    alphas, values = pl.pallas_call(
        finish,
        out_shape=(
            jax.ShapeDtypeStruct((BELIEFS, W), f32),
            jax.ShapeDtypeStruct((PLANES, W), f32),
        ),
        in_specs=[vmem, vmem],
        out_specs=(vmem, vmem),
        name="finish",
    )(final, parts)
    return alphas[None], values.reshape(1, BELIEFS)


def solution(mesh):
    return jax.shard_map(
        local,
        mesh=mesh,
        in_specs=(
            P("section", None, "state"),
            P("section", None),
            P("section", None, None),
            P(None, None, "state"),
            P(None, "state", None),
            P(None, "state"),
            P(None, "state"),
        ),
        out_specs=(P("section", None, "state"), P("section", None)),
        check_vma=False,
    )
```

```python
import jax
import jax.numpy as jnp
from jax import lax
from jax.experimental import pallas as pl
from jax.experimental.pallas import tpu as pltpu
from jax.sharding import PartitionSpec as P

MESH = pl.DeviceIdType.MESH
discount = 0.95

ACTIONS = 8
OBS = 32
STEPS = 8
SECTIONS = 8
PLANES = 4
CHIPS = 8
SHARDS = 16
BELIEFS = 512
BATCH = 128
ROWS = 64
W = 128
FOLD = 256
TAB = 40
GROUP = 8
GROUPS = ((0, 1), (2, 3, 4, 5), (6, 7))
LAST = STEPS - 1
DIRECT = 1


def kernel(
    next_hbm, action_hbm, reward_hbm, obs_hbm, terminal_hbm, trans_hbm, belief_hbm,
    final, vbuf,
    next_ref, action_ref, reward_ref, obs, trans, belief, nbuf, tab, idx, turned, onehot, weight, reward, rewrow, masked,
    pair_send, pair_recv, part_send, part_recv, fresh,
    bel, vsend, own_ssem, own_rsem, load_sem, bel_ssem, bel_rsem, idx_ssem, idx_rsem, reward_ssem, reward_rsem, pair_ssem, pair_rsem, part_ssem, part_rsem,
    row_ssem, row_rsem, out_ssem, out_rsem, val_ssem, val_rsem,
):
    sec = lax.axis_index("section")
    st = lax.axis_index("state")
    plane, half = lax.rem(sec, PLANES), lax.div(sec, PLANES)
    core, chip = lax.rem(st, 2), lax.div(st, 2)
    lo, y = lax.div(chip, 4), lax.rem(chip, 4)

    mine = plane * 2 + half

    def rows_of(m):
        return pl.ds(pl.multiple_of(m * ROWS, ROWS), ROWS)

    def other_section(d):
        return lax.rem(sec + d, SECTIONS)

    def other_state(d):
        return lax.rem(st + d, SHARDS)

    def z_neighbour(up, d):
        z = lax.rem(half * 2 + lo + (1 if up else 3), 4)
        return {
            "section": lax.div(z, 2) * PLANES + lax.rem(plane + d, PLANES),
            "state": (lax.rem(z, 2) * 4 + y) * 2 + core,
        }

    loads = [
        pltpu.make_async_copy(obs_hbm, obs, load_sem.at[0]),
        pltpu.make_async_copy(terminal_hbm, nbuf.at[0], load_sem.at[1]),
        pltpu.make_async_copy(trans_hbm, trans, load_sem.at[2]),
        pltpu.make_async_copy(belief_hbm, belief, load_sem.at[3]),
    ]
    small = [
        pltpu.make_async_copy(next_hbm, next_ref, load_sem.at[4]),
        pltpu.make_async_copy(action_hbm, action_ref, load_sem.at[5]),
        pltpu.make_async_copy(reward_hbm, reward_ref, load_sem.at[6]),
    ]
    for load in small:
        load.start()

    barrier = pltpu.get_barrier_semaphore()
    for d in range(1, SECTIONS):
        pl.semaphore_signal(barrier, inc=1, device_id={"section": other_section(d), "state": st}, device_id_type=MESH)
    for d in range(1, SHARDS):
        pl.semaphore_signal(barrier, inc=1, device_id={"section": sec, "state": other_state(d)}, device_id_type=MESH)
    for up in (True, False):
        for d in range(PLANES):
            pl.semaphore_signal(barrier, inc=1, device_id=z_neighbour(up, d), device_id_type=MESH)

    for load in loads:
        load.start()
    for load in small:
        load.wait()

    for p in range(PLANES):
        tab[p, 0:OBS, :] = next_ref[:, p * BATCH : (p + 1) * BATCH]
        tab[p, OBS : OBS + 1, :] = action_ref[:, p * BATCH : (p + 1) * BATCH]
        tab[p, OBS + 1 :, :] = jnp.zeros((TAB - OBS - 1, BATCH), jnp.int32)
        for t in range(1, STEPS):
            @pl.when(p > plane)
            def _():
                nbuf[t, p * BATCH : (p + 1) * BATCH, :] = jnp.zeros((BATCH, W), jnp.float32)
    idx[pl.ds(sec, 1)] = tab[pl.ds(plane, 1)]

    pl.semaphore_wait(barrier, SECTIONS - 1 + SHARDS - 1 + 2 * PLANES)

    def idx_copy(d):
        to = other_section(d)
        return pltpu.make_async_remote_copy(
            src_ref=tab.at[lax.rem(to, PLANES)], dst_ref=idx.at[sec],
            send_sem=idx_ssem.at[d], recv_sem=idx_rsem.at[sec],
            device_id={"section": to, "state": st}, device_id_type=MESH,
        )

    @pl.when(sec == SECTIONS - 1)
    def _():
        for d in (1, 5, 2, 6, 3, 7, 4):
            idx_copy(d).start()

    reward_copy = pltpu.make_async_remote_copy(
        src_ref=reward_ref, dst_ref=reward, send_sem=reward_ssem, recv_sem=reward_rsem,
        device_id=z_neighbour(True, 0), device_id_type=MESH,
    )
    reward_copy.start()

    def prepare(t):
        h = STEPS - 1 - t

        @pl.when(h != sec)
        def _():
            pltpu.make_async_remote_copy(
                src_ref=idx.at[h], dst_ref=idx.at[h], send_sem=idx_ssem.at[0], recv_sem=idx_rsem.at[h],
                device_id={"section": sec, "state": other_state(1)}, device_id_type=MESH,
            ).wait_recv()

        turned[...] = idx[h].T
        table = turned[pl.ds(pl.multiple_of(half * ROWS, ROWS), ROWS), :]
        act = table[:, OBS : OBS + 1]
        row = jnp.zeros((ROWS, W), jnp.float32)
        for a in range(ACTIONS):
            row = jnp.where(act == a, reward[a : a + 1, :], row)
        rewrow[lax.rem(t, 2)] = row
        wide = jnp.broadcast_to(act, (ROWS, W))
        column = lax.broadcasted_iota(jnp.int32, (ROWS, FOLD), 1)
        for o in range(OBS):
            pick = table[:, o : o + 1]
            onehot[o * ROWS : (o + 1) * ROWS, :] = (
                jnp.where(column == lax.rem(pick, FOLD), 1.0, 0.0).astype(jnp.bfloat16)
            )
            w = jnp.zeros((ROWS, W), jnp.float32)
            for a in range(ACTIONS):
                w = jnp.where(wide == a, obs[a, o : o + 1, :], w)
            upper = jnp.broadcast_to(pick >= FOLD, (ROWS, W))
            weight[o, :, :W] = jnp.where(upper, 0.0, w)
            weight[o, :, W:] = jnp.where(upper, w, 0.0)

    order = ((1, 2), (0, 2), (1, 1), (1, 3), (0, 1), (0, 3), (1, 0), (0, 0))

    def chip_at(k, flip):
        return lax.rem(lo + order[k][0] + flip, 2) * 4 + lax.rem(y + order[k][1], 4)

    def pair_copy(k, t):
        return pltpu.make_async_remote_copy(
            src_ref=pair_send.at[k], dst_ref=pair_recv.at[t, k],
            send_sem=pair_ssem.at[k], recv_sem=pair_rsem.at[t, k],
            device_id={"section": sec, "state": chip * 2 + 1 - core}, device_id_type=MESH,
        )

    def part_copy(k, t):
        return pltpu.make_async_remote_copy(
            src_ref=part_send.at[k], dst_ref=part_recv.at[t, k],
            send_sem=part_ssem.at[k], recv_sem=part_rsem.at[t, k],
            device_id={"section": sec, "state": chip_at(k, 0) * 2 + core}, device_id_type=MESH,
        )

    def cross_copy(k, t):
        return pltpu.make_async_remote_copy(
            src_ref=pair_send.at[k], dst_ref=part_recv.at[t, CHIPS + k],
            send_sem=pair_ssem.at[k], recv_sem=part_rsem.at[t, CHIPS + k],
            device_id={"section": sec, "state": chip_at(k, 0) * 2 + 1 - core}, device_id_type=MESH,
        )

    users = tuple((d, up) for d in range(PLANES) for up in (True, False))

    def row_copy(u, t):
        d, up = users[u]
        return pltpu.make_async_remote_copy(
            src_ref=fresh.at[t], dst_ref=nbuf.at[t + 1, rows_of(mine)],
            send_sem=row_ssem.at[u], recv_sem=row_rsem.at[t, mine],
            device_id=z_neighbour(up, d), device_id_type=MESH,
        )

    def feeds(u, t):
        return (plane + users[u][0] < PLANES) & (t < STEPS - 1)

    def out_copy(t):
        return pltpu.make_async_remote_copy(
            src_ref=fresh.at[t], dst_ref=final.at[rows_of(mine)],
            send_sem=out_ssem, recv_sem=out_rsem.at[mine],
            device_id={"section": STEPS - 1 - t, "state": ((1 - lo) * 4 + y) * 2 + core},
            device_id_type=MESH,
        )

    def goes_out(t):
        return (lax.rem(STEPS - 1 - t, PLANES) < plane) | (t == STEPS - 1)

    def bel_copy(m):
        return pltpu.make_async_remote_copy(
            src_ref=belief.at[m * ROWS : (m + 1) * ROWS], dst_ref=bel,
            send_sem=bel_ssem.at[m], recv_sem=bel_rsem,
            device_id={"section": (m % 2) * PLANES + m // 2, "state": ((1 - lo) * 4 + y) * 2 + core},
            device_id_type=MESH,
        )

    def own_val_copy(s):
        return pltpu.make_async_remote_copy(
            src_ref=vsend, dst_ref=vbuf.at[st, pl.ds(mine, 1)], send_sem=own_ssem.at[s], recv_sem=own_rsem.at[mine],
            device_id={"section": 0, "state": s}, device_id_type=MESH,
        )

    def elsewhere(s):
        return (sec > 0) | (st != s)

    def wait_into(dst, sem):
        pltpu.make_async_remote_copy(
            src_ref=fresh.at[0], dst_ref=dst, send_sem=out_ssem, recv_sem=sem,
            device_id=z_neighbour(True, 0), device_id_type=MESH,
        ).wait_recv()

    def wait_sent(t):
        for u in range(len(users)):
            @pl.when(feeds(u, t))
            def _():
                row_copy(u, t).wait_send()

        @pl.when(goes_out(t))
        def _():
            out_copy(t).wait_send()

    loads[0].wait()
    reward_copy.wait_recv()
    prepare(0)

    @pl.when(sec < SECTIONS - 1)
    def _():
        for d in range(1, SECTIONS):
            idx_copy(d).start()

    loads[1].wait()
    loads[2].wait()

    def step(t, carry):
        following = nbuf[t].astype(jnp.bfloat16)
        folded = jnp.concatenate([following[:FOLD], following[FOLD:]], axis=1)
        total = jnp.zeros((ROWS, 2 * W), jnp.float32)
        for c in range(OBS // GROUP):
            got = jnp.dot(
                onehot[c * GROUP * ROWS : (c + 1) * GROUP * ROWS, :], folded,
                preferred_element_type=jnp.float32,
            ).reshape(GROUP, ROWS, 2 * W)
            total = total + jnp.sum(got * weight[c * GROUP : (c + 1) * GROUP], axis=0)
        total = total[:, :W] + total[:, W:]
        act = turned[pl.ds(pl.multiple_of(half * ROWS, ROWS), ROWS), :][:, OBS : OBS + 1]
        for a in range(ACTIONS):
            masked[:, a * W : (a + 1) * W] = jnp.where(act == a, total, 0.0).astype(jnp.bfloat16)

        for group in GROUPS:
            parts = [
                jnp.dot(
                    masked[...], trans[:, pl.ds(pl.multiple_of(chip_at(k, 1) * 2 * W, 2 * W), 2 * W)],
                    preferred_element_type=jnp.float32,
                )
                for k in group
            ]
            for k, part in zip(group, parts):
                pair_send[k] = jnp.where(core == 0, part[:, W:], part[:, :W])
                part_send[k] = jnp.where(core == 0, part[:, :W], part[:, W:])
            for k in group:
                if k < DIRECT:
                    part_copy(k, t).start()
                    cross_copy(k, t).start()
                else:
                    pair_copy(k, t).start()
        for k in range(DIRECT, CHIPS):
            pair_copy(k, t).wait_recv()
            part_send[k] = part_send[k] + pair_recv[t, k]
            if k < CHIPS - 1:
                part_copy(k, t).start()

        @pl.when(t > 0)
        def _():
            wait_sent(t - 1)

        @pl.when(t < STEPS - 1)
        def _():
            prepare(t + 1)

        for k in range(DIRECT):
            cross_copy(k, t).wait_send()
        for k in range(DIRECT, CHIPS):
            pair_copy(k, t).wait_send()
        summed = part_send[CHIPS - 1]
        for k in range(DIRECT):
            cross_copy(k, t).wait_recv()
            summed = summed + part_recv[t, CHIPS + k]
        for k in range(CHIPS - 1):
            part_copy(k, t).wait_recv()
            summed = summed + part_recv[t, k]
        fresh[t] = rewrow[lax.rem(t, 2)] + discount * summed
        for u in range(len(users)):
            @pl.when(feeds(u, t))
            def _():
                row_copy(u, t).start()

        @pl.when(goes_out(t))
        def _():
            out_copy(t).start()

        @pl.when((t == LAST - 2) & (sec == 0))
        def _():
            loads[3].wait()
            for m in range(2 * PLANES):
                bel_copy(m).start()

        @pl.when(t == LAST)
        def _():
            bel_copy(0).wait_recv()
            product = fresh[t] * bel[...]
            nothing = jnp.zeros((ROWS, W), jnp.float32)
            first = jnp.concatenate([product, nothing], axis=0)
            second = jnp.concatenate([nothing, product], axis=0)
            both = jnp.where(half == 0, first, second)
            vsend[...] = jnp.sum(both.T, axis=0, keepdims=True)
            for s in range(SHARDS):
                @pl.when(elsewhere(s))
                def _():
                    own_val_copy(s).start()

        for k in range(CHIPS - 1):
            part_copy(k, t).wait_send()

        @pl.when(t < STEPS - 1)
        def _():
            for m in range(2 * PLANES):
                @pl.when(m // 2 <= plane)
                def _():
                    wait_into(nbuf.at[t + 1, rows_of(m)], row_rsem.at[t, m])

        return carry

    lax.fori_loop(0, STEPS, step, 0)

    own = STEPS - 1 - sec

    @pl.when(sec > 0)
    def _():
        loads[3].wait()

    for p in range(PLANES):
        used = (p <= plane) & (sec > 0)

        @pl.when(used)
        def _():
            final[p * BATCH : (p + 1) * BATCH, :] = nbuf[own + 1, p * BATCH : (p + 1) * BATCH, :]

        @pl.when(jnp.logical_not(used))
        def _():
            for m in (2 * p, 2 * p + 1):
                wait_into(final.at[rows_of(m)], out_rsem.at[m])

    def val_copy(d):
        return pltpu.make_async_remote_copy(
            src_ref=vbuf.at[st], dst_ref=vbuf.at[st],
            send_sem=val_ssem.at[d], recv_sem=val_rsem.at[d],
            device_id={"section": sec, "state": other_state(d)}, device_id_type=MESH,
        )

    @pl.when(sec > 0)
    def _():
        for p in range(PLANES):
            block = final[p * BATCH : (p + 1) * BATCH, :] * belief[p * BATCH : (p + 1) * BATCH, :]
            vbuf[pl.ds(st, 1), 2 * p : 2 * p + 1, :] = jnp.sum(block.T, axis=0, keepdims=True)[None]
            vbuf[pl.ds(st, 1), 2 * p + 1 : 2 * p + 2, :] = jnp.zeros((1, 1, W), jnp.float32)
        for d in range(1, SHARDS):
            val_copy(d).start()

    @pl.when(sec == 0)
    def _():
        vbuf[pl.ds(st, 1), 0:1, :] = vsend[...][None]
        for m in range(2 * PLANES):
            count = SHARDS if m else SHARDS - 1
            pltpu.make_async_remote_copy(
                src_ref=vbuf.at[pl.ds(0, count), m], dst_ref=vbuf.at[pl.ds(0, count), m],
                send_sem=own_ssem.at[0], recv_sem=own_rsem.at[m],
                device_id=z_neighbour(True, 0), device_id_type=MESH,
            ).wait_recv()

    wait_sent(STEPS - 1)
    reward_copy.wait_send()
    for d in range(1, SECTIONS):
        idx_copy(d).wait_send()
    for s in range(SHARDS):
        @pl.when(elsewhere(s))
        def _():
            own_val_copy(s).wait_send()

    @pl.when(sec == 0)
    def _():
        for m in range(2 * PLANES):
            bel_copy(m).wait_send()

    @pl.when(sec > 0)
    def _():
        for d in range(1, SHARDS):
            val_copy(d).wait_recv()
        for d in range(1, SHARDS):
            val_copy(d).wait_send()


def finish(final_ref, vbuf_ref, alphas_hbm, values_ref, sem):
    out = pltpu.make_async_copy(final_ref, alphas_hbm, sem)
    out.start()
    value = vbuf_ref[0]
    for s in range(1, SHARDS):
        value = value + vbuf_ref[s]
    for p in range(PLANES):
        values_ref[p : p + 1, :] = value[2 * p : 2 * p + 1, :] + value[2 * p + 1 : 2 * p + 2, :]
    out.wait()


def local(belief, action, next_index, obs_table, transition, reward, terminal):
    vmem = pl.BlockSpec(memory_space=pltpu.VMEM)
    anywhere = pl.BlockSpec(memory_space=pl.ANY)
    dma = pltpu.SemaphoreType.DMA
    f32 = jnp.float32
    final, parts = pl.pallas_call(
        kernel,
        out_shape=(
            pltpu.VMEM((BELIEFS, W), f32),
            pltpu.VMEM((SHARDS, 2 * PLANES, W), f32),
        ),
        in_specs=[anywhere] * 7,
        out_specs=(vmem, vmem),
        scratch_shapes=[
            pltpu.VMEM((OBS, BELIEFS), jnp.int32),
            pltpu.VMEM((1, BELIEFS), jnp.int32),
            pltpu.VMEM((ACTIONS, W), f32),
            pltpu.VMEM((ACTIONS, OBS, W), f32),
            pltpu.VMEM((ACTIONS * W, SHARDS * W), jnp.bfloat16),
            pltpu.VMEM((BELIEFS, W), f32),
            pltpu.VMEM((STEPS + 1, BELIEFS, W), f32),
            pltpu.VMEM((PLANES, TAB, BATCH), jnp.int32),
            pltpu.VMEM((SECTIONS, TAB, BATCH), jnp.int32),
            pltpu.VMEM((BATCH, TAB), jnp.int32),
            pltpu.VMEM((OBS * ROWS, FOLD), jnp.bfloat16),
            pltpu.VMEM((OBS, ROWS, 2 * W), f32),
            pltpu.VMEM((ACTIONS, W), f32),
            pltpu.VMEM((2, ROWS, W), f32),
            pltpu.VMEM((ROWS, ACTIONS * W), jnp.bfloat16),
            pltpu.VMEM((CHIPS, ROWS, W), f32),
            pltpu.VMEM((STEPS, CHIPS, ROWS, W), f32),
            pltpu.VMEM((CHIPS, ROWS, W), f32),
            pltpu.VMEM((STEPS, CHIPS + DIRECT, ROWS, W), f32),
            pltpu.VMEM((STEPS, ROWS, W), f32),
            pltpu.VMEM((ROWS, W), f32),
            pltpu.VMEM((1, W), f32),
            dma((SHARDS,)),
            dma((2 * PLANES,)),
            dma((7,)),
            dma((2 * PLANES,)),
            dma,
            dma((SECTIONS,)),
            dma((SECTIONS,)),
            dma,
            dma,
            dma((CHIPS,)),
            dma((STEPS, CHIPS)),
            dma((CHIPS,)),
            dma((STEPS, CHIPS + DIRECT)),
            dma((2 * PLANES,)),
            dma((STEPS, 2 * PLANES)),
            dma,
            dma((2 * PLANES,)),
            dma((SHARDS,)),
            dma((SHARDS,)),
        ],
        compiler_params=pltpu.CompilerParams(
            collective_id=0, has_side_effects=True, vmem_limit_bytes=60 * 1024 * 1024
        ),
        name="chain",
    )(
        next_index[0].T, action, reward, obs_table, terminal,
        transition.reshape(ACTIONS * W, SHARDS * W), belief[0],
    )
    alphas, values = pl.pallas_call(
        finish,
        out_shape=(
            jax.ShapeDtypeStruct((BELIEFS, W), f32),
            jax.ShapeDtypeStruct((PLANES, W), f32),
        ),
        in_specs=[vmem, vmem],
        out_specs=(anywhere, vmem),
        scratch_shapes=[dma],
        name="finish",
    )(
        pltpu.with_memory_space_constraint(final, pltpu.VMEM),
        pltpu.with_memory_space_constraint(parts, pltpu.VMEM),
    )
    return alphas[None], values.reshape(1, BELIEFS)


def solution(mesh):
    return jax.shard_map(
        local,
        mesh=mesh,
        in_specs=(
            P("section", None, "state"),
            P("section", None),
            P("section", None, None),
            P(None, None, "state"),
            P(None, "state", None),
            P(None, "state"),
            P(None, "state"),
        ),
        out_specs=(P("section", None, "state"), P("section", None)),
        check_vma=False,
    )
```

```python
import jax
import jax.numpy as jnp
from jax import lax
from jax.experimental import pallas as pl
from jax.experimental.pallas import tpu as pltpu
from jax.sharding import PartitionSpec as P

MESH = pl.DeviceIdType.MESH
discount = 0.95

ACTIONS = 8
OBS = 32
STEPS = 8
SECTIONS = 8
PLANES = 4
CHIPS = 8
SHARDS = 16
BELIEFS = 512
BATCH = 128
ROWS = 64
W = 128
FOLD = 256
TAB = 40
GROUP = 8
GROUPS = ((0, 1), (2, 3, 4, 5), (6, 7))
LAST = STEPS - 1
OWN = 2 * (PLANES - 1)
DIRECT = 1


def kernel(
    next_hbm, action_hbm, reward_hbm, obs_hbm, terminal_hbm, trans_hbm, belief_hbm,
    final, vbuf,
    next_ref, action_ref, reward_ref, obs, trans, belief, nbuf, tab, idx, turned, onehot, weight, reward, rewrow, masked,
    pair_send, pair_recv, part_send, part_recv, fresh,
    bel, vsend, own_ssem, own_rsem, load_sem, bel_ssem, bel_rsem, idx_ssem, idx_rsem, reward_ssem, reward_rsem, pair_ssem, pair_rsem, part_ssem, part_rsem,
    row_ssem, row_rsem, out_ssem, out_rsem, val_ssem, val_rsem,
):
    sec = lax.axis_index("section")
    st = lax.axis_index("state")
    plane, half = PLANES - 1 - lax.rem(sec, PLANES), lax.div(sec, PLANES)
    core, chip = lax.rem(st, 2), lax.div(st, 2)
    lo, y = lax.div(chip, 4), lax.rem(chip, 4)

    mine = plane * 2 + half

    def rows_of(m):
        return pl.ds(pl.multiple_of(m * ROWS, ROWS), ROWS)

    def other_section(d):
        return lax.rem(sec + d, SECTIONS)

    def other_state(d):
        return lax.rem(st + d, SHARDS)

    def z_neighbour(up, d):
        z = lax.rem(half * 2 + lo + (1 if up else 3), 4)
        return {
            "section": lax.div(z, 2) * PLANES + PLANES - 1 - lax.rem(plane + d, PLANES),
            "state": (lax.rem(z, 2) * 4 + y) * 2 + core,
        }

    loads = [
        pltpu.make_async_copy(obs_hbm, obs, load_sem.at[0]),
        pltpu.make_async_copy(terminal_hbm, nbuf.at[0], load_sem.at[1]),
        pltpu.make_async_copy(trans_hbm, trans, load_sem.at[2]),
        pltpu.make_async_copy(belief_hbm, belief, load_sem.at[3]),
    ]
    small = [
        pltpu.make_async_copy(next_hbm, next_ref, load_sem.at[4]),
        pltpu.make_async_copy(action_hbm, action_ref, load_sem.at[5]),
        pltpu.make_async_copy(reward_hbm, reward_ref, load_sem.at[6]),
    ]
    for load in small:
        load.start()

    barrier = pltpu.get_barrier_semaphore()
    for d in range(1, SECTIONS):
        pl.semaphore_signal(barrier, inc=1, device_id={"section": other_section(d), "state": st}, device_id_type=MESH)
    for d in range(1, SHARDS):
        pl.semaphore_signal(barrier, inc=1, device_id={"section": sec, "state": other_state(d)}, device_id_type=MESH)
    for up in (True, False):
        for d in range(PLANES):
            pl.semaphore_signal(barrier, inc=1, device_id=z_neighbour(up, d), device_id_type=MESH)

    for load in loads:
        load.start()
    for load in small:
        load.wait()

    for p in range(PLANES):
        tab[p, 0:OBS, :] = next_ref[:, p * BATCH : (p + 1) * BATCH]
        tab[p, OBS : OBS + 1, :] = action_ref[:, p * BATCH : (p + 1) * BATCH]
        tab[p, OBS + 1 :, :] = jnp.zeros((TAB - OBS - 1, BATCH), jnp.int32)
        for t in range(1, STEPS):
            @pl.when(p > plane)
            def _():
                nbuf[t, p * BATCH : (p + 1) * BATCH, :] = jnp.zeros((BATCH, W), jnp.float32)
    idx[pl.ds(sec, 1)] = tab[pl.ds(plane, 1)]

    pl.semaphore_wait(barrier, SECTIONS - 1 + SHARDS - 1 + 2 * PLANES)

    def idx_copy(d):
        to = other_section(d)
        return pltpu.make_async_remote_copy(
            src_ref=tab.at[PLANES - 1 - lax.rem(to, PLANES)], dst_ref=idx.at[sec],
            send_sem=idx_ssem.at[d], recv_sem=idx_rsem.at[sec],
            device_id={"section": to, "state": st}, device_id_type=MESH,
        )

    @pl.when(sec == SECTIONS - 1)
    def _():
        for d in (4, 7, 3, 6, 2, 5, 1):
            idx_copy(d).start()

    reward_copy = pltpu.make_async_remote_copy(
        src_ref=reward_ref, dst_ref=reward, send_sem=reward_ssem, recv_sem=reward_rsem,
        device_id=z_neighbour(True, 0), device_id_type=MESH,
    )
    reward_copy.start()

    def prepare(t):
        h = STEPS - 1 - t

        @pl.when(h != sec)
        def _():
            pltpu.make_async_remote_copy(
                src_ref=idx.at[h], dst_ref=idx.at[h], send_sem=idx_ssem.at[0], recv_sem=idx_rsem.at[h],
                device_id={"section": sec, "state": other_state(1)}, device_id_type=MESH,
            ).wait_recv()

        turned[...] = idx[h].T
        table = turned[pl.ds(pl.multiple_of(half * ROWS, ROWS), ROWS), :]
        act = table[:, OBS : OBS + 1]
        row = jnp.zeros((ROWS, W), jnp.float32)
        for a in range(ACTIONS):
            row = jnp.where(act == a, reward[a : a + 1, :], row)
        rewrow[lax.rem(t, 2)] = row
        wide = jnp.broadcast_to(act, (ROWS, W))
        column = lax.broadcasted_iota(jnp.int32, (ROWS, FOLD), 1)
        for o in range(OBS):
            pick = table[:, o : o + 1]
            onehot[o * ROWS : (o + 1) * ROWS, :] = (
                jnp.where(column == lax.rem(pick, FOLD), 1.0, 0.0).astype(jnp.bfloat16)
            )
            w = jnp.zeros((ROWS, W), jnp.float32)
            for a in range(ACTIONS):
                w = jnp.where(wide == a, obs[a, o : o + 1, :], w)
            upper = jnp.broadcast_to(pick >= FOLD, (ROWS, W))
            weight[o, :, :W] = jnp.where(upper, 0.0, w)
            weight[o, :, W:] = jnp.where(upper, w, 0.0)

    order = ((1, 2), (0, 2), (1, 1), (1, 3), (0, 1), (0, 3), (1, 0), (0, 0))

    def chip_at(k, flip):
        return lax.rem(lo + order[k][0] + flip, 2) * 4 + lax.rem(y + order[k][1], 4)

    def pair_copy(k, t):
        return pltpu.make_async_remote_copy(
            src_ref=pair_send.at[k], dst_ref=pair_recv.at[t, k],
            send_sem=pair_ssem.at[k], recv_sem=pair_rsem.at[t, k],
            device_id={"section": sec, "state": chip * 2 + 1 - core}, device_id_type=MESH,
        )

    def part_copy(k, t):
        return pltpu.make_async_remote_copy(
            src_ref=part_send.at[k], dst_ref=part_recv.at[t, k],
            send_sem=part_ssem.at[k], recv_sem=part_rsem.at[t, k],
            device_id={"section": sec, "state": chip_at(k, 0) * 2 + core}, device_id_type=MESH,
        )

    def cross_copy(k, t):
        return pltpu.make_async_remote_copy(
            src_ref=pair_send.at[k], dst_ref=part_recv.at[t, CHIPS + k],
            send_sem=pair_ssem.at[k], recv_sem=part_rsem.at[t, CHIPS + k],
            device_id={"section": sec, "state": chip_at(k, 0) * 2 + 1 - core}, device_id_type=MESH,
        )

    users = tuple((d, up) for d in (1, 0, 3, 2) for up in (True, False))

    def row_copy(u, t):
        d, up = users[u]
        return pltpu.make_async_remote_copy(
            src_ref=fresh.at[t], dst_ref=nbuf.at[t + 1, rows_of(mine)],
            send_sem=row_ssem.at[u], recv_sem=row_rsem.at[t, mine],
            device_id=z_neighbour(up, d), device_id_type=MESH,
        )

    def feeds(u, t):
        return (plane + users[u][0] < PLANES) & (t < STEPS - 1)

    def out_copy(t):
        return pltpu.make_async_remote_copy(
            src_ref=fresh.at[t], dst_ref=final.at[rows_of(mine)],
            send_sem=out_ssem, recv_sem=out_rsem.at[mine],
            device_id={"section": STEPS - 1 - t, "state": ((1 - lo) * 4 + y) * 2 + core},
            device_id_type=MESH,
        )

    def goes_out(t):
        return (PLANES - 1 - lax.rem(STEPS - 1 - t, PLANES) < plane) | (t == STEPS - 1)

    def bel_copy(m):
        return pltpu.make_async_remote_copy(
            src_ref=belief.at[m * ROWS : (m + 1) * ROWS], dst_ref=bel,
            send_sem=bel_ssem.at[m], recv_sem=bel_rsem,
            device_id={"section": (m % 2) * PLANES + PLANES - 1 - m // 2, "state": ((1 - lo) * 4 + y) * 2 + core},
            device_id_type=MESH,
        )

    def own_val_copy(s):
        return pltpu.make_async_remote_copy(
            src_ref=vsend, dst_ref=vbuf.at[st, pl.ds(mine, 1)], send_sem=own_ssem.at[s], recv_sem=own_rsem.at[mine],
            device_id={"section": 0, "state": s}, device_id_type=MESH,
        )

    def elsewhere(s):
        return (sec > 0) | (st != s)

    def wait_into(dst, sem):
        pltpu.make_async_remote_copy(
            src_ref=fresh.at[0], dst_ref=dst, send_sem=out_ssem, recv_sem=sem,
            device_id=z_neighbour(True, 0), device_id_type=MESH,
        ).wait_recv()

    def wait_sent(t):
        for u in range(len(users)):
            @pl.when(feeds(u, t))
            def _():
                row_copy(u, t).wait_send()

        @pl.when(goes_out(t))
        def _():
            out_copy(t).wait_send()

    loads[0].wait()
    reward_copy.wait_recv()
    prepare(0)

    @pl.when(sec < SECTIONS - 1)
    def _():
        for d in range(1, SECTIONS):
            idx_copy(d).start()

    loads[1].wait()
    loads[2].wait()

    def step(t, carry):
        following = nbuf[t].astype(jnp.bfloat16)
        folded = jnp.concatenate([following[:FOLD], following[FOLD:]], axis=1)
        total = jnp.zeros((ROWS, 2 * W), jnp.float32)
        for c in range(OBS // GROUP):
            got = jnp.dot(
                onehot[c * GROUP * ROWS : (c + 1) * GROUP * ROWS, :], folded,
                preferred_element_type=jnp.float32,
            ).reshape(GROUP, ROWS, 2 * W)
            total = total + jnp.sum(got * weight[c * GROUP : (c + 1) * GROUP], axis=0)
        total = total[:, :W] + total[:, W:]
        act = turned[pl.ds(pl.multiple_of(half * ROWS, ROWS), ROWS), :][:, OBS : OBS + 1]
        for a in range(ACTIONS):
            masked[:, a * W : (a + 1) * W] = jnp.where(act == a, total, 0.0).astype(jnp.bfloat16)

        for group in GROUPS:
            parts = [
                jnp.dot(
                    masked[...], trans[:, pl.ds(pl.multiple_of(chip_at(k, 1) * 2 * W, 2 * W), 2 * W)],
                    preferred_element_type=jnp.float32,
                )
                for k in group
            ]
            for k, part in zip(group, parts):
                pair_send[k] = jnp.where(core == 0, part[:, W:], part[:, :W])
                part_send[k] = jnp.where(core == 0, part[:, :W], part[:, W:])
            for k in group:
                if k < DIRECT:
                    part_copy(k, t).start()
                    cross_copy(k, t).start()
                else:
                    pair_copy(k, t).start()
        for k in range(DIRECT, CHIPS):
            pair_copy(k, t).wait_recv()
            part_send[k] = part_send[k] + pair_recv[t, k]
            if k < CHIPS - 1:
                part_copy(k, t).start()

        @pl.when(t > 0)
        def _():
            wait_sent(t - 1)

        @pl.when(t < STEPS - 1)
        def _():
            prepare(t + 1)

        for k in range(DIRECT):
            cross_copy(k, t).wait_send()
        for k in range(DIRECT, CHIPS):
            pair_copy(k, t).wait_send()
        summed = part_send[CHIPS - 1]
        for k in range(DIRECT):
            cross_copy(k, t).wait_recv()
            summed = summed + part_recv[t, CHIPS + k]
        for k in range(CHIPS - 1):
            part_copy(k, t).wait_recv()
            summed = summed + part_recv[t, k]
        fresh[t] = rewrow[lax.rem(t, 2)] + discount * summed
        for u in range(len(users)):
            @pl.when(feeds(u, t))
            def _():
                row_copy(u, t).start()

        @pl.when(goes_out(t))
        def _():
            out_copy(t).start()

        @pl.when((t == 1) & (sec == 0))
        def _():
            loads[3].wait()
            for m in range(2 * PLANES):
                bel_copy(m).start()

        @pl.when(t == LAST)
        def _():
            bel_copy(0).wait_recv()
            product = fresh[t] * bel[...]
            nothing = jnp.zeros((ROWS, W), jnp.float32)
            first = jnp.concatenate([product, nothing], axis=0)
            second = jnp.concatenate([nothing, product], axis=0)
            both = jnp.where(half == 0, first, second)
            vsend[...] = jnp.sum(both.T, axis=0, keepdims=True)
            for s in range(SHARDS):
                @pl.when(elsewhere(s))
                def _():
                    own_val_copy(s).start()

        for k in range(CHIPS - 1):
            part_copy(k, t).wait_send()

        @pl.when(t < STEPS - 1)
        def _():
            for m in range(2 * PLANES):
                @pl.when(m // 2 <= plane)
                def _():
                    wait_into(nbuf.at[t + 1, rows_of(m)], row_rsem.at[t, m])

        return carry

    lax.fori_loop(0, STEPS, step, 0)

    own = STEPS - 1 - sec

    @pl.when(sec > 0)
    def _():
        loads[3].wait()

    for p in range(PLANES):
        used = (p <= plane) & (sec > 0)

        @pl.when(used)
        def _():
            final[p * BATCH : (p + 1) * BATCH, :] = nbuf[own + 1, p * BATCH : (p + 1) * BATCH, :]

        @pl.when(jnp.logical_not(used))
        def _():
            for m in (2 * p, 2 * p + 1):
                wait_into(final.at[rows_of(m)], out_rsem.at[m])

    def val_copy(d):
        return pltpu.make_async_remote_copy(
            src_ref=vbuf.at[st], dst_ref=vbuf.at[st],
            send_sem=val_ssem.at[d], recv_sem=val_rsem.at[d],
            device_id={"section": sec, "state": other_state(d)}, device_id_type=MESH,
        )

    @pl.when(sec > 0)
    def _():
        for p in range(PLANES):
            block = final[p * BATCH : (p + 1) * BATCH, :] * belief[p * BATCH : (p + 1) * BATCH, :]
            vbuf[pl.ds(st, 1), 2 * p : 2 * p + 1, :] = jnp.sum(block.T, axis=0, keepdims=True)[None]
            vbuf[pl.ds(st, 1), 2 * p + 1 : 2 * p + 2, :] = jnp.zeros((1, 1, W), jnp.float32)
        for d in range(1, SHARDS):
            val_copy(d).start()

    @pl.when(sec == 0)
    def _():
        vbuf[pl.ds(st, 1), OWN : OWN + 1, :] = vsend[...][None]
        for m in range(2 * PLANES):
            count = SHARDS - 1 if m == OWN else SHARDS
            pltpu.make_async_remote_copy(
                src_ref=vbuf.at[pl.ds(0, count), m], dst_ref=vbuf.at[pl.ds(0, count), m],
                send_sem=own_ssem.at[0], recv_sem=own_rsem.at[m],
                device_id=z_neighbour(True, 0), device_id_type=MESH,
            ).wait_recv()

    wait_sent(STEPS - 1)
    reward_copy.wait_send()
    for d in range(1, SECTIONS):
        idx_copy(d).wait_send()
    for s in range(SHARDS):
        @pl.when(elsewhere(s))
        def _():
            own_val_copy(s).wait_send()

    @pl.when(sec == 0)
    def _():
        for m in range(2 * PLANES):
            bel_copy(m).wait_send()

    @pl.when(sec > 0)
    def _():
        for d in range(1, SHARDS):
            val_copy(d).wait_recv()
        for d in range(1, SHARDS):
            val_copy(d).wait_send()


def finish(final_ref, vbuf_ref, alphas_ref, values_ref):
    alphas_ref[...] = final_ref[...]
    value = vbuf_ref[0]
    for s in range(1, SHARDS):
        value = value + vbuf_ref[s]
    for p in range(PLANES):
        values_ref[p : p + 1, :] = value[2 * p : 2 * p + 1, :] + value[2 * p + 1 : 2 * p + 2, :]


def local(belief, action, next_index, obs_table, transition, reward, terminal):
    vmem = pl.BlockSpec(memory_space=pltpu.VMEM)
    anywhere = pl.BlockSpec(memory_space=pl.ANY)
    dma = pltpu.SemaphoreType.DMA
    f32 = jnp.float32
    final, parts = pl.pallas_call(
        kernel,
        out_shape=(
            pltpu.VMEM((BELIEFS, W), f32),
            pltpu.VMEM((SHARDS, 2 * PLANES, W), f32),
        ),
        in_specs=[anywhere] * 7,
        out_specs=(vmem, vmem),
        scratch_shapes=[
            pltpu.VMEM((OBS, BELIEFS), jnp.int32),
            pltpu.VMEM((1, BELIEFS), jnp.int32),
            pltpu.VMEM((ACTIONS, W), f32),
            pltpu.VMEM((ACTIONS, OBS, W), f32),
            pltpu.VMEM((ACTIONS * W, SHARDS * W), jnp.bfloat16),
            pltpu.VMEM((BELIEFS, W), f32),
            pltpu.VMEM((STEPS + 1, BELIEFS, W), f32),
            pltpu.VMEM((PLANES, TAB, BATCH), jnp.int32),
            pltpu.VMEM((SECTIONS, TAB, BATCH), jnp.int32),
            pltpu.VMEM((BATCH, TAB), jnp.int32),
            pltpu.VMEM((OBS * ROWS, FOLD), jnp.bfloat16),
            pltpu.VMEM((OBS, ROWS, 2 * W), f32),
            pltpu.VMEM((ACTIONS, W), f32),
            pltpu.VMEM((2, ROWS, W), f32),
            pltpu.VMEM((ROWS, ACTIONS * W), jnp.bfloat16),
            pltpu.VMEM((CHIPS, ROWS, W), f32),
            pltpu.VMEM((STEPS, CHIPS, ROWS, W), f32),
            pltpu.VMEM((CHIPS, ROWS, W), f32),
            pltpu.VMEM((STEPS, CHIPS + DIRECT, ROWS, W), f32),
            pltpu.VMEM((STEPS, ROWS, W), f32),
            pltpu.VMEM((ROWS, W), f32),
            pltpu.VMEM((1, W), f32),
            dma((SHARDS,)),
            dma((2 * PLANES,)),
            dma((7,)),
            dma((2 * PLANES,)),
            dma,
            dma((SECTIONS,)),
            dma((SECTIONS,)),
            dma,
            dma,
            dma((CHIPS,)),
            dma((STEPS, CHIPS)),
            dma((CHIPS,)),
            dma((STEPS, CHIPS + DIRECT)),
            dma((2 * PLANES,)),
            dma((STEPS, 2 * PLANES)),
            dma,
            dma((2 * PLANES,)),
            dma((SHARDS,)),
            dma((SHARDS,)),
        ],
        compiler_params=pltpu.CompilerParams(
            collective_id=0, has_side_effects=True, vmem_limit_bytes=60 * 1024 * 1024
        ),
        name="chain",
    )(
        next_index[0].T, action, reward, obs_table, terminal,
        transition.reshape(ACTIONS * W, SHARDS * W), belief[0],
    )
    alphas, values = pl.pallas_call(
        finish,
        out_shape=(
            jax.ShapeDtypeStruct((BELIEFS, W), f32),
            jax.ShapeDtypeStruct((PLANES, W), f32),
        ),
        in_specs=[vmem, vmem],
        out_specs=(vmem, vmem),
        name="finish",
    )(
        pltpu.with_memory_space_constraint(final, pltpu.VMEM),
        pltpu.with_memory_space_constraint(parts, pltpu.VMEM),
    )
    return alphas[None], values.reshape(1, BELIEFS)


def solution(mesh):
    return jax.shard_map(
        local,
        mesh=mesh,
        in_specs=(
            P("section", None, "state"),
            P("section", None),
            P("section", None, None),
            P(None, None, "state"),
            P(None, "state", None),
            P(None, "state"),
            P(None, "state"),
        ),
        out_specs=(P("section", None, "state"), P("section", None)),
        check_vma=False,
    )
```

```python
import jax
import jax.numpy as jnp
from jax import lax
from jax.experimental import pallas as pl
from jax.experimental.pallas import tpu as pltpu
from jax.sharding import PartitionSpec as P

MESH = pl.DeviceIdType.MESH
discount = 0.95

ACTIONS = 8
OBS = 32
STEPS = 8
SECTIONS = 8
PLANES = 4
CHIPS = 8
SHARDS = 16
BELIEFS = 512
BATCH = 128
ROWS = 64
W = 128
FOLD = 256
TAB = 40
GROUP = 8
GROUPS = ((0, 1), (2, 3, 4, 5), (6, 7))
LAST = STEPS - 1
OWN = 2 * (PLANES - 1)
DIRECT = 1


def kernel(
    next_hbm, action_hbm, reward_hbm, obs_hbm, terminal_hbm, trans_hbm, belief_hbm,
    final, vbuf,
    next_ref, action_ref, reward_ref, obs, trans, belief, nbuf, tab, idx, turned, onehot, weight, reward, rewrow, masked,
    pair_send, pair_recv, part_send, part_recv, fresh,
    bel, vsend, own_ssem, own_rsem, load_sem, bel_ssem, bel_rsem, idx_ssem, idx_rsem, reward_ssem, reward_rsem, pair_ssem, pair_rsem, part_ssem, part_rsem,
    row_ssem, row_rsem, out_ssem, out_rsem, val_ssem, val_rsem,
):
    sec = lax.axis_index("section")
    st = lax.axis_index("state")
    plane, half = PLANES - 1 - lax.rem(sec, PLANES), lax.div(sec, PLANES)
    core, chip = lax.rem(st, 2), lax.div(st, 2)
    lo, y = lax.div(chip, 4), lax.rem(chip, 4)

    mine = plane * 2 + half

    def rows_of(m):
        return pl.ds(pl.multiple_of(m * ROWS, ROWS), ROWS)

    def other_section(d):
        return lax.rem(sec + d, SECTIONS)

    def other_state(d):
        return lax.rem(st + d, SHARDS)

    def z_neighbour(up, d):
        z = lax.rem(half * 2 + lo + (1 if up else 3), 4)
        return {
            "section": lax.div(z, 2) * PLANES + PLANES - 1 - lax.rem(plane + d, PLANES),
            "state": (lax.rem(z, 2) * 4 + y) * 2 + core,
        }

    loads = [
        pltpu.make_async_copy(obs_hbm, obs, load_sem.at[0]),
        pltpu.make_async_copy(terminal_hbm, nbuf.at[0], load_sem.at[1]),
        pltpu.make_async_copy(trans_hbm, trans, load_sem.at[2]),
        pltpu.make_async_copy(belief_hbm, belief, load_sem.at[3]),
    ]
    small = [
        pltpu.make_async_copy(next_hbm, next_ref, load_sem.at[4]),
        pltpu.make_async_copy(action_hbm, action_ref, load_sem.at[5]),
        pltpu.make_async_copy(reward_hbm, reward_ref, load_sem.at[6]),
    ]
    for load in small:
        load.start()

    barrier = pltpu.get_barrier_semaphore()
    for d in range(1, SECTIONS):
        pl.semaphore_signal(barrier, inc=1, device_id={"section": other_section(d), "state": st}, device_id_type=MESH)
    for d in range(1, SHARDS):
        pl.semaphore_signal(barrier, inc=1, device_id={"section": sec, "state": other_state(d)}, device_id_type=MESH)
    for up in (True, False):
        for d in range(PLANES):
            pl.semaphore_signal(barrier, inc=1, device_id=z_neighbour(up, d), device_id_type=MESH)

    for load in loads:
        load.start()
    for load in small:
        load.wait()

    for p in range(PLANES):
        tab[p, 0:OBS, :] = next_ref[:, p * BATCH : (p + 1) * BATCH]
        tab[p, OBS : OBS + 1, :] = action_ref[:, p * BATCH : (p + 1) * BATCH]
        tab[p, OBS + 1 :, :] = jnp.zeros((TAB - OBS - 1, BATCH), jnp.int32)
        for t in range(1, STEPS):
            @pl.when(p > plane)
            def _():
                nbuf[t, p * BATCH : (p + 1) * BATCH, :] = jnp.zeros((BATCH, W), jnp.float32)
    idx[pl.ds(sec, 1)] = tab[pl.ds(plane, 1)]

    pl.semaphore_wait(barrier, SECTIONS - 1 + SHARDS - 1 + 2 * PLANES)

    def idx_copy(d):
        to = other_section(d)
        return pltpu.make_async_remote_copy(
            src_ref=tab.at[PLANES - 1 - lax.rem(to, PLANES)], dst_ref=idx.at[sec],
            send_sem=idx_ssem.at[d], recv_sem=idx_rsem.at[sec],
            device_id={"section": to, "state": st}, device_id_type=MESH,
        )

    @pl.when(sec == SECTIONS - 1)
    def _():
        for d in (4, 7, 3, 6, 2, 5, 1):
            idx_copy(d).start()

    reward_copy = pltpu.make_async_remote_copy(
        src_ref=reward_ref, dst_ref=reward, send_sem=reward_ssem, recv_sem=reward_rsem,
        device_id=z_neighbour(True, 0), device_id_type=MESH,
    )
    reward_copy.start()

    def prepare(t):
        h = STEPS - 1 - t

        @pl.when(h != sec)
        def _():
            pltpu.make_async_remote_copy(
                src_ref=idx.at[h], dst_ref=idx.at[h], send_sem=idx_ssem.at[0], recv_sem=idx_rsem.at[h],
                device_id={"section": sec, "state": other_state(1)}, device_id_type=MESH,
            ).wait_recv()

        turned[...] = idx[h].T
        table = turned[pl.ds(pl.multiple_of(half * ROWS, ROWS), ROWS), :]
        act = table[:, OBS : OBS + 1]
        row = jnp.zeros((ROWS, W), jnp.float32)
        for a in range(ACTIONS):
            row = jnp.where(act == a, reward[a : a + 1, :], row)
        rewrow[lax.rem(t, 2)] = row
        wide = jnp.broadcast_to(act, (ROWS, W))
        column = lax.broadcasted_iota(jnp.int32, (ROWS, FOLD), 1)
        for o in range(OBS):
            pick = table[:, o : o + 1]
            onehot[o * ROWS : (o + 1) * ROWS, :] = (
                jnp.where(column == lax.rem(pick, FOLD), 1.0, 0.0).astype(jnp.bfloat16)
            )
            w = jnp.zeros((ROWS, W), jnp.float32)
            for a in range(ACTIONS):
                w = jnp.where(wide == a, obs[a, o : o + 1, :], w)
            upper = jnp.broadcast_to(pick >= FOLD, (ROWS, W))
            weight[o, :, :W] = jnp.where(upper, 0.0, w)
            weight[o, :, W:] = jnp.where(upper, w, 0.0)

    order = ((1, 2), (1, 1), (1, 3), (0, 2), (1, 0), (0, 1), (0, 3), (0, 0))

    def chip_at(k, flip):
        return lax.rem(lo + order[k][0] + flip, 2) * 4 + lax.rem(y + order[k][1], 4)

    def pair_copy(k, t):
        return pltpu.make_async_remote_copy(
            src_ref=pair_send.at[k], dst_ref=pair_recv.at[t, k],
            send_sem=pair_ssem.at[k], recv_sem=pair_rsem.at[t, k],
            device_id={"section": sec, "state": chip * 2 + 1 - core}, device_id_type=MESH,
        )

    def part_copy(k, t):
        return pltpu.make_async_remote_copy(
            src_ref=part_send.at[k], dst_ref=part_recv.at[t, k],
            send_sem=part_ssem.at[k], recv_sem=part_rsem.at[t, k],
            device_id={"section": sec, "state": chip_at(k, 0) * 2 + core}, device_id_type=MESH,
        )

    def cross_copy(k, t):
        return pltpu.make_async_remote_copy(
            src_ref=pair_send.at[k], dst_ref=part_recv.at[t, CHIPS + k],
            send_sem=pair_ssem.at[k], recv_sem=part_rsem.at[t, CHIPS + k],
            device_id={"section": sec, "state": chip_at(k, 0) * 2 + 1 - core}, device_id_type=MESH,
        )

    users = tuple((d, up) for d in (1, 0, 3, 2) for up in (True, False))

    def row_copy(u, t):
        d, up = users[u]
        return pltpu.make_async_remote_copy(
            src_ref=fresh.at[t], dst_ref=nbuf.at[t + 1, rows_of(mine)],
            send_sem=row_ssem.at[u], recv_sem=row_rsem.at[t, mine],
            device_id=z_neighbour(up, d), device_id_type=MESH,
        )

    def feeds(u, t):
        return (plane + users[u][0] < PLANES) & (t < STEPS - 1)

    def out_copy(t):
        return pltpu.make_async_remote_copy(
            src_ref=fresh.at[t], dst_ref=final.at[rows_of(mine)],
            send_sem=out_ssem, recv_sem=out_rsem.at[mine],
            device_id={"section": STEPS - 1 - t, "state": ((1 - lo) * 4 + y) * 2 + core},
            device_id_type=MESH,
        )

    def goes_out(t):
        return (PLANES - 1 - lax.rem(STEPS - 1 - t, PLANES) < plane) | (t == STEPS - 1)

    def bel_copy(m):
        return pltpu.make_async_remote_copy(
            src_ref=belief.at[m * ROWS : (m + 1) * ROWS], dst_ref=bel,
            send_sem=bel_ssem.at[m], recv_sem=bel_rsem,
            device_id={"section": (m % 2) * PLANES + PLANES - 1 - m // 2, "state": ((1 - lo) * 4 + y) * 2 + core},
            device_id_type=MESH,
        )

    def own_val_copy(s):
        return pltpu.make_async_remote_copy(
            src_ref=vsend, dst_ref=vbuf.at[st, pl.ds(mine, 1)], send_sem=own_ssem.at[s], recv_sem=own_rsem.at[mine],
            device_id={"section": 0, "state": s}, device_id_type=MESH,
        )

    def elsewhere(s):
        return (sec > 0) | (st != s)

    def wait_into(dst, sem):
        pltpu.make_async_remote_copy(
            src_ref=fresh.at[0], dst_ref=dst, send_sem=out_ssem, recv_sem=sem,
            device_id=z_neighbour(True, 0), device_id_type=MESH,
        ).wait_recv()

    def wait_sent(t):
        for u in range(len(users)):
            @pl.when(feeds(u, t))
            def _():
                row_copy(u, t).wait_send()

        @pl.when(goes_out(t))
        def _():
            out_copy(t).wait_send()

    loads[0].wait()
    reward_copy.wait_recv()
    prepare(0)

    @pl.when(sec < SECTIONS - 1)
    def _():
        for d in range(1, SECTIONS):
            idx_copy(d).start()

    loads[1].wait()
    loads[2].wait()

    def step(t, carry):
        following = nbuf[t].astype(jnp.bfloat16)
        folded = jnp.concatenate([following[:FOLD], following[FOLD:]], axis=1)
        total = jnp.zeros((ROWS, 2 * W), jnp.float32)
        for c in range(OBS // GROUP):
            got = jnp.dot(
                onehot[c * GROUP * ROWS : (c + 1) * GROUP * ROWS, :], folded,
                preferred_element_type=jnp.float32,
            ).reshape(GROUP, ROWS, 2 * W)
            total = total + jnp.sum(got * weight[c * GROUP : (c + 1) * GROUP], axis=0)
        total = total[:, :W] + total[:, W:]
        act = turned[pl.ds(pl.multiple_of(half * ROWS, ROWS), ROWS), :][:, OBS : OBS + 1]
        for a in range(ACTIONS):
            masked[:, a * W : (a + 1) * W] = jnp.where(act == a, total, 0.0).astype(jnp.bfloat16)

        for group in GROUPS:
            parts = [
                jnp.dot(
                    masked[...], trans[:, pl.ds(pl.multiple_of(chip_at(k, 1) * 2 * W, 2 * W), 2 * W)],
                    preferred_element_type=jnp.float32,
                )
                for k in group
            ]
            for k, part in zip(group, parts):
                pair_send[k] = jnp.where(core == 0, part[:, W:], part[:, :W])
                part_send[k] = jnp.where(core == 0, part[:, :W], part[:, W:])
            for k in group:
                if k < DIRECT:
                    part_copy(k, t).start()
                    cross_copy(k, t).start()
                else:
                    pair_copy(k, t).start()
        for k in range(DIRECT, CHIPS):
            pair_copy(k, t).wait_recv()
            part_send[k] = part_send[k] + pair_recv[t, k]
            if k < CHIPS - 1:
                part_copy(k, t).start()

        @pl.when(t > 0)
        def _():
            wait_sent(t - 1)

        @pl.when(t < STEPS - 1)
        def _():
            prepare(t + 1)

        for k in range(DIRECT):
            cross_copy(k, t).wait_send()
        for k in range(DIRECT, CHIPS):
            pair_copy(k, t).wait_send()
        summed = part_send[CHIPS - 1]
        for k in range(DIRECT):
            cross_copy(k, t).wait_recv()
            summed = summed + part_recv[t, CHIPS + k]
        for k in range(CHIPS - 1):
            part_copy(k, t).wait_recv()
            summed = summed + part_recv[t, k]
        fresh[t] = rewrow[lax.rem(t, 2)] + discount * summed
        for u in range(len(users)):
            @pl.when(feeds(u, t))
            def _():
                row_copy(u, t).start()

        @pl.when(goes_out(t))
        def _():
            out_copy(t).start()

        @pl.when((t == 1) & (sec == 0))
        def _():
            loads[3].wait()
            for m in range(2 * PLANES):
                bel_copy(m).start()

        @pl.when(t == LAST)
        def _():
            bel_copy(0).wait_recv()
            product = fresh[t] * bel[...]
            nothing = jnp.zeros((ROWS, W), jnp.float32)
            first = jnp.concatenate([product, nothing], axis=0)
            second = jnp.concatenate([nothing, product], axis=0)
            both = jnp.where(half == 0, first, second)
            vsend[...] = jnp.sum(both.T, axis=0, keepdims=True)
            for s in range(SHARDS):
                @pl.when(elsewhere(s))
                def _():
                    own_val_copy(s).start()

        for k in range(CHIPS - 1):
            part_copy(k, t).wait_send()

        @pl.when(t < STEPS - 1)
        def _():
            for m in range(2 * PLANES):
                @pl.when(m // 2 <= plane)
                def _():
                    wait_into(nbuf.at[t + 1, rows_of(m)], row_rsem.at[t, m])

        return carry

    lax.fori_loop(0, STEPS, step, 0)

    own = STEPS - 1 - sec

    @pl.when(sec > 0)
    def _():
        loads[3].wait()

    for p in range(PLANES):
        used = (p <= plane) & (sec > 0)

        @pl.when(used)
        def _():
            final[p * BATCH : (p + 1) * BATCH, :] = nbuf[own + 1, p * BATCH : (p + 1) * BATCH, :]

        @pl.when(jnp.logical_not(used))
        def _():
            for m in (2 * p, 2 * p + 1):
                wait_into(final.at[rows_of(m)], out_rsem.at[m])

    def val_copy(d):
        return pltpu.make_async_remote_copy(
            src_ref=vbuf.at[st], dst_ref=vbuf.at[st],
            send_sem=val_ssem.at[d], recv_sem=val_rsem.at[d],
            device_id={"section": sec, "state": other_state(d)}, device_id_type=MESH,
        )

    @pl.when(sec > 0)
    def _():
        for p in range(PLANES):
            block = final[p * BATCH : (p + 1) * BATCH, :] * belief[p * BATCH : (p + 1) * BATCH, :]
            vbuf[pl.ds(st, 1), 2 * p : 2 * p + 1, :] = jnp.sum(block.T, axis=0, keepdims=True)[None]
            vbuf[pl.ds(st, 1), 2 * p + 1 : 2 * p + 2, :] = jnp.zeros((1, 1, W), jnp.float32)
        for d in range(1, SHARDS):
            val_copy(d).start()

    @pl.when(sec == 0)
    def _():
        vbuf[pl.ds(st, 1), OWN : OWN + 1, :] = vsend[...][None]
        for m in range(2 * PLANES):
            count = SHARDS - 1 if m == OWN else SHARDS
            pltpu.make_async_remote_copy(
                src_ref=vbuf.at[pl.ds(0, count), m], dst_ref=vbuf.at[pl.ds(0, count), m],
                send_sem=own_ssem.at[0], recv_sem=own_rsem.at[m],
                device_id=z_neighbour(True, 0), device_id_type=MESH,
            ).wait_recv()

    wait_sent(STEPS - 1)
    reward_copy.wait_send()
    for d in range(1, SECTIONS):
        idx_copy(d).wait_send()
    for s in range(SHARDS):
        @pl.when(elsewhere(s))
        def _():
            own_val_copy(s).wait_send()

    @pl.when(sec == 0)
    def _():
        for m in range(2 * PLANES):
            bel_copy(m).wait_send()

    @pl.when(sec > 0)
    def _():
        for d in range(1, SHARDS):
            val_copy(d).wait_recv()
        for d in range(1, SHARDS):
            val_copy(d).wait_send()


def finish(final_ref, vbuf_ref, alphas_ref, values_ref):
    alphas_ref[...] = final_ref[...]
    value = vbuf_ref[0]
    for s in range(1, SHARDS):
        value = value + vbuf_ref[s]
    for p in range(PLANES):
        values_ref[p : p + 1, :] = value[2 * p : 2 * p + 1, :] + value[2 * p + 1 : 2 * p + 2, :]


def local(belief, action, next_index, obs_table, transition, reward, terminal):
    vmem = pl.BlockSpec(memory_space=pltpu.VMEM)
    anywhere = pl.BlockSpec(memory_space=pl.ANY)
    dma = pltpu.SemaphoreType.DMA
    f32 = jnp.float32
    final, parts = pl.pallas_call(
        kernel,
        out_shape=(
            pltpu.VMEM((BELIEFS, W), f32),
            pltpu.VMEM((SHARDS, 2 * PLANES, W), f32),
        ),
        in_specs=[anywhere] * 7,
        out_specs=(vmem, vmem),
        scratch_shapes=[
            pltpu.VMEM((OBS, BELIEFS), jnp.int32),
            pltpu.VMEM((1, BELIEFS), jnp.int32),
            pltpu.VMEM((ACTIONS, W), f32),
            pltpu.VMEM((ACTIONS, OBS, W), f32),
            pltpu.VMEM((ACTIONS * W, SHARDS * W), jnp.bfloat16),
            pltpu.VMEM((BELIEFS, W), f32),
            pltpu.VMEM((STEPS + 1, BELIEFS, W), f32),
            pltpu.VMEM((PLANES, TAB, BATCH), jnp.int32),
            pltpu.VMEM((SECTIONS, TAB, BATCH), jnp.int32),
            pltpu.VMEM((BATCH, TAB), jnp.int32),
            pltpu.VMEM((OBS * ROWS, FOLD), jnp.bfloat16),
            pltpu.VMEM((OBS, ROWS, 2 * W), f32),
            pltpu.VMEM((ACTIONS, W), f32),
            pltpu.VMEM((2, ROWS, W), f32),
            pltpu.VMEM((ROWS, ACTIONS * W), jnp.bfloat16),
            pltpu.VMEM((CHIPS, ROWS, W), f32),
            pltpu.VMEM((STEPS, CHIPS, ROWS, W), f32),
            pltpu.VMEM((CHIPS, ROWS, W), f32),
            pltpu.VMEM((STEPS, CHIPS + DIRECT, ROWS, W), f32),
            pltpu.VMEM((STEPS, ROWS, W), f32),
            pltpu.VMEM((ROWS, W), f32),
            pltpu.VMEM((1, W), f32),
            dma((SHARDS,)),
            dma((2 * PLANES,)),
            dma((7,)),
            dma((2 * PLANES,)),
            dma,
            dma((SECTIONS,)),
            dma((SECTIONS,)),
            dma,
            dma,
            dma((CHIPS,)),
            dma((STEPS, CHIPS)),
            dma((CHIPS,)),
            dma((STEPS, CHIPS + DIRECT)),
            dma((2 * PLANES,)),
            dma((STEPS, 2 * PLANES)),
            dma,
            dma((2 * PLANES,)),
            dma((SHARDS,)),
            dma((SHARDS,)),
        ],
        compiler_params=pltpu.CompilerParams(
            collective_id=0, has_side_effects=True, vmem_limit_bytes=60 * 1024 * 1024
        ),
        name="chain",
    )(
        next_index[0].T, action, reward, obs_table, terminal,
        transition.reshape(ACTIONS * W, SHARDS * W), belief[0],
    )
    alphas, values = pl.pallas_call(
        finish,
        out_shape=(
            jax.ShapeDtypeStruct((BELIEFS, W), f32),
            jax.ShapeDtypeStruct((PLANES, W), f32),
        ),
        in_specs=[vmem, vmem],
        out_specs=(vmem, vmem),
        name="finish",
    )(
        pltpu.with_memory_space_constraint(final, pltpu.VMEM),
        pltpu.with_memory_space_constraint(parts, pltpu.VMEM),
    )
    return alphas[None], values.reshape(1, BELIEFS)


def solution(mesh):
    return jax.shard_map(
        local,
        mesh=mesh,
        in_specs=(
            P("section", None, "state"),
            P("section", None),
            P("section", None, None),
            P(None, None, "state"),
            P(None, "state", None),
            P(None, "state"),
            P(None, "state"),
        ),
        out_specs=(P("section", None, "state"), P("section", None)),
        check_vma=False,
    )
```

```python
import jax
import jax.numpy as jnp
from jax import lax
from jax.experimental import pallas as pl
from jax.experimental.pallas import tpu as pltpu
from jax.sharding import PartitionSpec as P

MESH = pl.DeviceIdType.MESH
discount = 0.95

ACTIONS = 8
OBS = 32
STEPS = 8
SECTIONS = 8
PLANES = 4
CHIPS = 8
SHARDS = 16
BELIEFS = 512
BATCH = 128
ROWS = 64
W = 128
FOLD = 256
TAB = 40
GROUP = 8
GROUPS = ((0, 1), (2, 3, 4, 5), (6, 7))
LAST = STEPS - 1
OWN = 2 * (PLANES - 1)
DIRECT = 1


def kernel(
    next_hbm, action_hbm, reward_hbm, obs_hbm, terminal_hbm, trans_hbm, belief_hbm,
    final, vbuf,
    next_ref, action_ref, reward_ref, obs, trans, belief, nbuf, tab, idx, turned, onehot, weight, reward, rewrow, masked,
    pair_send, pair_recv, part_send, part_recv, fresh,
    bel, vsend, own_ssem, own_rsem, load_sem, bel_ssem, bel_rsem, idx_ssem, idx_rsem, reward_ssem, reward_rsem, pair_ssem, pair_rsem, part_ssem, part_rsem,
    row_ssem, row_rsem, out_ssem, out_rsem, val_ssem, val_rsem,
):
    sec = lax.axis_index("section")
    st = lax.axis_index("state")
    plane, half = PLANES - 1 - lax.rem(sec, PLANES), lax.div(sec, PLANES)
    core, chip = lax.rem(st, 2), lax.div(st, 2)
    lo, y = lax.div(chip, 4), lax.rem(chip, 4)

    mine = plane * 2 + half

    def rows_of(m):
        return pl.ds(pl.multiple_of(m * ROWS, ROWS), ROWS)

    def other_section(d):
        return lax.rem(sec + d, SECTIONS)

    def other_state(d):
        return lax.rem(st + d, SHARDS)

    def z_neighbour(up, d):
        z = lax.rem(half * 2 + lo + (1 if up else 3), 4)
        return {
            "section": lax.div(z, 2) * PLANES + PLANES - 1 - lax.rem(plane + d, PLANES),
            "state": (lax.rem(z, 2) * 4 + y) * 2 + core,
        }

    loads = [
        pltpu.make_async_copy(obs_hbm, obs, load_sem.at[0]),
        pltpu.make_async_copy(terminal_hbm, nbuf.at[0], load_sem.at[1]),
        pltpu.make_async_copy(trans_hbm, trans, load_sem.at[2]),
        pltpu.make_async_copy(belief_hbm, belief, load_sem.at[3]),
    ]
    small = [
        pltpu.make_async_copy(next_hbm, next_ref, load_sem.at[4]),
        pltpu.make_async_copy(action_hbm, action_ref, load_sem.at[5]),
        pltpu.make_async_copy(reward_hbm, reward_ref, load_sem.at[6]),
    ]
    for load in small:
        load.start()

    barrier = pltpu.get_barrier_semaphore()
    for d in range(1, SECTIONS):
        pl.semaphore_signal(barrier, inc=1, device_id={"section": other_section(d), "state": st}, device_id_type=MESH)
    for d in range(1, SHARDS):
        pl.semaphore_signal(barrier, inc=1, device_id={"section": sec, "state": other_state(d)}, device_id_type=MESH)
    for up in (True, False):
        for d in range(PLANES):
            pl.semaphore_signal(barrier, inc=1, device_id=z_neighbour(up, d), device_id_type=MESH)

    for load in loads:
        load.start()
    for load in small:
        load.wait()

    for p in range(PLANES):
        tab[p, 0:OBS, :] = next_ref[:, p * BATCH : (p + 1) * BATCH]
        tab[p, OBS : OBS + 1, :] = action_ref[:, p * BATCH : (p + 1) * BATCH]
        tab[p, OBS + 1 :, :] = jnp.zeros((TAB - OBS - 1, BATCH), jnp.int32)
        for t in range(1, STEPS):
            @pl.when(p > plane)
            def _():
                nbuf[t, p * BATCH : (p + 1) * BATCH, :] = jnp.zeros((BATCH, W), jnp.float32)
    idx[pl.ds(sec, 1)] = tab[pl.ds(plane, 1)]

    pl.semaphore_wait(barrier, SECTIONS - 1 + SHARDS - 1 + 2 * PLANES)

    def idx_copy(d):
        to = other_section(d)
        return pltpu.make_async_remote_copy(
            src_ref=tab.at[PLANES - 1 - lax.rem(to, PLANES)], dst_ref=idx.at[sec],
            send_sem=idx_ssem.at[d], recv_sem=idx_rsem.at[sec],
            device_id={"section": to, "state": st}, device_id_type=MESH,
        )

    @pl.when(sec == SECTIONS - 1)
    def _():
        for d in (4, 7, 3, 6, 2, 5, 1):
            idx_copy(d).start()

    reward_copy = pltpu.make_async_remote_copy(
        src_ref=reward_ref, dst_ref=reward, send_sem=reward_ssem, recv_sem=reward_rsem,
        device_id=z_neighbour(True, 0), device_id_type=MESH,
    )
    reward_copy.start()

    def prepare(t):
        h = STEPS - 1 - t

        @pl.when(h != sec)
        def _():
            pltpu.make_async_remote_copy(
                src_ref=idx.at[h], dst_ref=idx.at[h], send_sem=idx_ssem.at[0], recv_sem=idx_rsem.at[h],
                device_id={"section": sec, "state": other_state(1)}, device_id_type=MESH,
            ).wait_recv()

        turned[...] = idx[h].T
        table = turned[pl.ds(pl.multiple_of(half * ROWS, ROWS), ROWS), :]
        act = table[:, OBS : OBS + 1]
        row = jnp.zeros((ROWS, W), jnp.float32)
        for a in range(ACTIONS):
            row = jnp.where(act == a, reward[a : a + 1, :], row)
        rewrow[lax.rem(t, 2)] = row
        wide = jnp.broadcast_to(act, (ROWS, W))
        column = lax.broadcasted_iota(jnp.int32, (ROWS, FOLD), 1)
        for o in range(OBS):
            pick = table[:, o : o + 1]
            onehot[o * ROWS : (o + 1) * ROWS, :] = (
                jnp.where(column == lax.rem(pick, FOLD), 1.0, 0.0).astype(jnp.bfloat16)
            )
            w = jnp.zeros((ROWS, W), jnp.float32)
            for a in range(ACTIONS):
                w = jnp.where(wide == a, obs[a, o : o + 1, :], w)
            upper = jnp.broadcast_to(pick >= FOLD, (ROWS, W))
            weight[o, :, :W] = jnp.where(upper, 0.0, w)
            weight[o, :, W:] = jnp.where(upper, w, 0.0)

    order = ((1, 2), (1, 0), (1, 1), (1, 3), (0, 2), (0, 1), (0, 3), (0, 0))

    def chip_at(k, flip):
        return lax.rem(lo + order[k][0] + flip, 2) * 4 + lax.rem(y + order[k][1], 4)

    def pair_copy(k, t):
        return pltpu.make_async_remote_copy(
            src_ref=pair_send.at[k], dst_ref=pair_recv.at[t, k],
            send_sem=pair_ssem.at[k], recv_sem=pair_rsem.at[t, k],
            device_id={"section": sec, "state": chip * 2 + 1 - core}, device_id_type=MESH,
        )

    def part_copy(k, t):
        return pltpu.make_async_remote_copy(
            src_ref=part_send.at[k], dst_ref=part_recv.at[t, k],
            send_sem=part_ssem.at[k], recv_sem=part_rsem.at[t, k],
            device_id={"section": sec, "state": chip_at(k, 0) * 2 + core}, device_id_type=MESH,
        )

    def cross_copy(k, t):
        return pltpu.make_async_remote_copy(
            src_ref=pair_send.at[k], dst_ref=part_recv.at[t, CHIPS + k],
            send_sem=pair_ssem.at[k], recv_sem=part_rsem.at[t, CHIPS + k],
            device_id={"section": sec, "state": chip_at(k, 0) * 2 + 1 - core}, device_id_type=MESH,
        )

    users = tuple((d, up) for d in (1, 0, 3, 2) for up in (True, False))

    def row_copy(u, t):
        d, up = users[u]
        return pltpu.make_async_remote_copy(
            src_ref=fresh.at[t], dst_ref=nbuf.at[t + 1, rows_of(mine)],
            send_sem=row_ssem.at[u], recv_sem=row_rsem.at[t, mine],
            device_id=z_neighbour(up, d), device_id_type=MESH,
        )

    def feeds(u, t):
        return (plane + users[u][0] < PLANES) & (t < STEPS - 1)

    def out_copy(t):
        return pltpu.make_async_remote_copy(
            src_ref=fresh.at[t], dst_ref=final.at[rows_of(mine)],
            send_sem=out_ssem, recv_sem=out_rsem.at[mine],
            device_id={"section": STEPS - 1 - t, "state": ((1 - lo) * 4 + y) * 2 + core},
            device_id_type=MESH,
        )

    def goes_out(t):
        return (PLANES - 1 - lax.rem(STEPS - 1 - t, PLANES) < plane) | (t == STEPS - 1)

    def bel_copy(m):
        return pltpu.make_async_remote_copy(
            src_ref=belief.at[m * ROWS : (m + 1) * ROWS], dst_ref=bel,
            send_sem=bel_ssem.at[m], recv_sem=bel_rsem,
            device_id={"section": (m % 2) * PLANES + PLANES - 1 - m // 2, "state": ((1 - lo) * 4 + y) * 2 + core},
            device_id_type=MESH,
        )

    def own_val_copy(s):
        return pltpu.make_async_remote_copy(
            src_ref=vsend, dst_ref=vbuf.at[st, pl.ds(mine, 1)], send_sem=own_ssem.at[s], recv_sem=own_rsem.at[mine],
            device_id={"section": 0, "state": s}, device_id_type=MESH,
        )

    def elsewhere(s):
        return (sec > 0) | (st != s)

    def wait_into(dst, sem):
        pltpu.make_async_remote_copy(
            src_ref=fresh.at[0], dst_ref=dst, send_sem=out_ssem, recv_sem=sem,
            device_id=z_neighbour(True, 0), device_id_type=MESH,
        ).wait_recv()

    def wait_sent(t):
        for u in range(len(users)):
            @pl.when(feeds(u, t))
            def _():
                row_copy(u, t).wait_send()

        @pl.when(goes_out(t))
        def _():
            out_copy(t).wait_send()

    loads[0].wait()
    reward_copy.wait_recv()
    prepare(0)

    @pl.when(sec < SECTIONS - 1)
    def _():
        for d in range(1, SECTIONS):
            idx_copy(d).start()

    loads[1].wait()
    loads[2].wait()

    def step(t, carry):
        following = nbuf[t].astype(jnp.bfloat16)
        folded = jnp.concatenate([following[:FOLD], following[FOLD:]], axis=1)
        total = jnp.zeros((ROWS, 2 * W), jnp.float32)
        for c in range(OBS // GROUP):
            got = jnp.dot(
                onehot[c * GROUP * ROWS : (c + 1) * GROUP * ROWS, :], folded,
                preferred_element_type=jnp.float32,
            ).reshape(GROUP, ROWS, 2 * W)
            total = total + jnp.sum(got * weight[c * GROUP : (c + 1) * GROUP], axis=0)
        total = total[:, :W] + total[:, W:]
        act = turned[pl.ds(pl.multiple_of(half * ROWS, ROWS), ROWS), :][:, OBS : OBS + 1]
        for a in range(ACTIONS):
            masked[:, a * W : (a + 1) * W] = jnp.where(act == a, total, 0.0).astype(jnp.bfloat16)

        for group in GROUPS:
            parts = [
                jnp.dot(
                    masked[...], trans[:, pl.ds(pl.multiple_of(chip_at(k, 1) * 2 * W, 2 * W), 2 * W)],
                    preferred_element_type=jnp.float32,
                )
                for k in group
            ]
            for k, part in zip(group, parts):
                pair_send[k] = jnp.where(core == 0, part[:, W:], part[:, :W])
                part_send[k] = jnp.where(core == 0, part[:, :W], part[:, W:])
            for k in group:
                if k < DIRECT:
                    part_copy(k, t).start()
                    cross_copy(k, t).start()
                else:
                    pair_copy(k, t).start()
        for k in range(DIRECT, CHIPS):
            pair_copy(k, t).wait_recv()
            part_send[k] = part_send[k] + pair_recv[t, k]
            if k < CHIPS - 1:
                part_copy(k, t).start()

        @pl.when(t > 0)
        def _():
            wait_sent(t - 1)

        @pl.when(t < STEPS - 1)
        def _():
            prepare(t + 1)

        for k in range(DIRECT):
            cross_copy(k, t).wait_send()
        for k in range(DIRECT, CHIPS):
            pair_copy(k, t).wait_send()
        summed = part_send[CHIPS - 1]
        for k in range(DIRECT):
            cross_copy(k, t).wait_recv()
            summed = summed + part_recv[t, CHIPS + k]
        for k in range(CHIPS - 1):
            part_copy(k, t).wait_recv()
            summed = summed + part_recv[t, k]
        fresh[t] = rewrow[lax.rem(t, 2)] + discount * summed
        for u in range(len(users)):
            @pl.when(feeds(u, t))
            def _():
                row_copy(u, t).start()

        @pl.when(goes_out(t))
        def _():
            out_copy(t).start()

        @pl.when((t == 1) & (sec == 0))
        def _():
            loads[3].wait()
            for m in range(2 * PLANES):
                bel_copy(m).start()

        @pl.when(t == LAST)
        def _():
            bel_copy(0).wait_recv()
            product = fresh[t] * bel[...]
            nothing = jnp.zeros((ROWS, W), jnp.float32)
            first = jnp.concatenate([product, nothing], axis=0)
            second = jnp.concatenate([nothing, product], axis=0)
            both = jnp.where(half == 0, first, second)
            vsend[...] = jnp.sum(both.T, axis=0, keepdims=True)
            for s in range(SHARDS):
                @pl.when(elsewhere(s))
                def _():
                    own_val_copy(s).start()

        for k in range(CHIPS - 1):
            part_copy(k, t).wait_send()

        @pl.when(t < STEPS - 1)
        def _():
            for m in range(2 * PLANES):
                @pl.when(m // 2 <= plane)
                def _():
                    wait_into(nbuf.at[t + 1, rows_of(m)], row_rsem.at[t, m])

        return carry

    lax.fori_loop(0, STEPS, step, 0)

    own = STEPS - 1 - sec

    @pl.when(sec > 0)
    def _():
        loads[3].wait()

    for p in range(PLANES):
        used = (p <= plane) & (sec > 0)

        @pl.when(used)
        def _():
            final[p * BATCH : (p + 1) * BATCH, :] = nbuf[own + 1, p * BATCH : (p + 1) * BATCH, :]

        @pl.when(jnp.logical_not(used))
        def _():
            for m in (2 * p, 2 * p + 1):
                wait_into(final.at[rows_of(m)], out_rsem.at[m])

    def val_copy(d):
        return pltpu.make_async_remote_copy(
            src_ref=vbuf.at[st], dst_ref=vbuf.at[st],
            send_sem=val_ssem.at[d], recv_sem=val_rsem.at[d],
            device_id={"section": sec, "state": other_state(d)}, device_id_type=MESH,
        )

    @pl.when(sec > 0)
    def _():
        for p in range(PLANES):
            block = final[p * BATCH : (p + 1) * BATCH, :] * belief[p * BATCH : (p + 1) * BATCH, :]
            vbuf[pl.ds(st, 1), 2 * p : 2 * p + 1, :] = jnp.sum(block.T, axis=0, keepdims=True)[None]
            vbuf[pl.ds(st, 1), 2 * p + 1 : 2 * p + 2, :] = jnp.zeros((1, 1, W), jnp.float32)
        for d in range(1, SHARDS):
            val_copy(d).start()

    @pl.when(sec == 0)
    def _():
        vbuf[pl.ds(st, 1), OWN : OWN + 1, :] = vsend[...][None]
        for m in range(2 * PLANES):
            count = SHARDS - 1 if m == OWN else SHARDS
            pltpu.make_async_remote_copy(
                src_ref=vbuf.at[pl.ds(0, count), m], dst_ref=vbuf.at[pl.ds(0, count), m],
                send_sem=own_ssem.at[0], recv_sem=own_rsem.at[m],
                device_id=z_neighbour(True, 0), device_id_type=MESH,
            ).wait_recv()

    wait_sent(STEPS - 1)
    reward_copy.wait_send()
    for d in range(1, SECTIONS):
        idx_copy(d).wait_send()
    for s in range(SHARDS):
        @pl.when(elsewhere(s))
        def _():
            own_val_copy(s).wait_send()

    @pl.when(sec == 0)
    def _():
        for m in range(2 * PLANES):
            bel_copy(m).wait_send()

    @pl.when(sec > 0)
    def _():
        for d in range(1, SHARDS):
            val_copy(d).wait_recv()
        for d in range(1, SHARDS):
            val_copy(d).wait_send()


def finish(final_ref, vbuf_ref, alphas_ref, values_ref):
    alphas_ref[...] = final_ref[...]
    value = vbuf_ref[0]
    for s in range(1, SHARDS):
        value = value + vbuf_ref[s]
    for p in range(PLANES):
        values_ref[p : p + 1, :] = value[2 * p : 2 * p + 1, :] + value[2 * p + 1 : 2 * p + 2, :]


def local(belief, action, next_index, obs_table, transition, reward, terminal):
    vmem = pl.BlockSpec(memory_space=pltpu.VMEM)
    anywhere = pl.BlockSpec(memory_space=pl.ANY)
    dma = pltpu.SemaphoreType.DMA
    f32 = jnp.float32
    final, parts = pl.pallas_call(
        kernel,
        out_shape=(
            pltpu.VMEM((BELIEFS, W), f32),
            pltpu.VMEM((SHARDS, 2 * PLANES, W), f32),
        ),
        in_specs=[anywhere] * 7,
        out_specs=(vmem, vmem),
        scratch_shapes=[
            pltpu.VMEM((OBS, BELIEFS), jnp.int32),
            pltpu.VMEM((1, BELIEFS), jnp.int32),
            pltpu.VMEM((ACTIONS, W), f32),
            pltpu.VMEM((ACTIONS, OBS, W), f32),
            pltpu.VMEM((ACTIONS * W, SHARDS * W), jnp.bfloat16),
            pltpu.VMEM((BELIEFS, W), f32),
            pltpu.VMEM((STEPS + 1, BELIEFS, W), f32),
            pltpu.VMEM((PLANES, TAB, BATCH), jnp.int32),
            pltpu.VMEM((SECTIONS, TAB, BATCH), jnp.int32),
            pltpu.VMEM((BATCH, TAB), jnp.int32),
            pltpu.VMEM((OBS * ROWS, FOLD), jnp.bfloat16),
            pltpu.VMEM((OBS, ROWS, 2 * W), f32),
            pltpu.VMEM((ACTIONS, W), f32),
            pltpu.VMEM((2, ROWS, W), f32),
            pltpu.VMEM((ROWS, ACTIONS * W), jnp.bfloat16),
            pltpu.VMEM((CHIPS, ROWS, W), f32),
            pltpu.VMEM((STEPS, CHIPS, ROWS, W), f32),
            pltpu.VMEM((CHIPS, ROWS, W), f32),
            pltpu.VMEM((STEPS, CHIPS + DIRECT, ROWS, W), f32),
            pltpu.VMEM((STEPS, ROWS, W), f32),
            pltpu.VMEM((ROWS, W), f32),
            pltpu.VMEM((1, W), f32),
            dma((SHARDS,)),
            dma((2 * PLANES,)),
            dma((7,)),
            dma((2 * PLANES,)),
            dma,
            dma((SECTIONS,)),
            dma((SECTIONS,)),
            dma,
            dma,
            dma((CHIPS,)),
            dma((STEPS, CHIPS)),
            dma((CHIPS,)),
            dma((STEPS, CHIPS + DIRECT)),
            dma((2 * PLANES,)),
            dma((STEPS, 2 * PLANES)),
            dma,
            dma((2 * PLANES,)),
            dma((SHARDS,)),
            dma((SHARDS,)),
        ],
        compiler_params=pltpu.CompilerParams(
            collective_id=0, has_side_effects=True, vmem_limit_bytes=60 * 1024 * 1024
        ),
        name="chain",
    )(
        next_index[0].T, action, reward, obs_table, terminal,
        transition.reshape(ACTIONS * W, SHARDS * W), belief[0],
    )
    alphas, values = pl.pallas_call(
        finish,
        out_shape=(
            jax.ShapeDtypeStruct((BELIEFS, W), f32),
            jax.ShapeDtypeStruct((PLANES, W), f32),
        ),
        in_specs=[vmem, vmem],
        out_specs=(vmem, vmem),
        name="finish",
    )(
        pltpu.with_memory_space_constraint(final, pltpu.VMEM),
        pltpu.with_memory_space_constraint(parts, pltpu.VMEM),
    )
    return alphas[None], values.reshape(1, BELIEFS)


def solution(mesh):
    return jax.shard_map(
        local,
        mesh=mesh,
        in_specs=(
            P("section", None, "state"),
            P("section", None),
            P("section", None, None),
            P(None, None, "state"),
            P(None, "state", None),
            P(None, "state"),
            P(None, "state"),
        ),
        out_specs=(P("section", None, "state"), P("section", None)),
        check_vma=False,
    )
```
